128 devices in a mesh: tm: 8 (over y, z_lo), freq: 16 (over x, z_hi, core).
Axes of the slice: x: 4, y: 4, z: 4 (z_hi: 2, z_lo: 2; z = z_hi * 2 + z_lo), core: 2. Of those that a mesh axis runs over, the one named last changes fastest.
Arguments:
- records: bfloat16 [1024, 1024, 512], P('freq', 'tm'), may hold values from -4 to 4
- gap_flags: int32 [1024, 32], P('freq', 'tm'), may hold values from -2147483648 to 2147483647
- station_mask: int32 [1024], P('freq'), may hold values 0 or 1
Outputs:
- cross_spectra: float32 [32, 2, 1024, 1024], P('freq', None, 'tm')
The draws below stay inside these ranges and needn't reach their ends.
All inputs are finite; a program needn't handle non-finite values. No bound on the sum of `station_mask` on one device may be relied on, other than what follows from the above.
Results may differ from the reference program's by a relative error of at most 0.0013.
Values may be sent and summed in bfloat16 or wider, within the bound.
A program may use at most 128 MiB of HBM per device.

```python
import math
import jax
import jax.numpy as jnp
from jax import lax

STATIONS = 1024
SAMPLES = 512
BAND = 32
WINDOWS = 1024


def draw_records(key, part):
    key_shared = jax.random.fold_in(key, 12)
    key_ambient = jax.random.fold_in(key, 13)
    key_silent = jax.random.fold_in(key, 14)
    silent = jax.random.uniform(key_silent, (STATIONS, WINDOWS, 1), jnp.float32) < 0.125
    shared = jax.random.normal(key_shared, (1, WINDOWS, SAMPLES), jnp.float32)
    ambient = jax.random.normal(key_ambient, (STATIONS, WINDOWS, SAMPLES), jnp.float32)
    values = 0.5 * shared + 0.866 * ambient
    values = jnp.where(silent, 0.0, values)
    return jnp.clip(values, -4.0, 4.0).astype(jnp.bfloat16)


def draw_gap_flags(key, part):
    key_station = jax.random.fold_in(key, 21)
    key_common = jax.random.fold_in(key, 22)
    station_clear = (jax.random.randint(key_station, (STATIONS, WINDOWS), 0, 20) >= 3).astype(jnp.int32)
    common_clear = (jax.random.randint(key_common, (1, WINDOWS), 0, 20) >= 3).astype(jnp.int32)
    flag_grid = (station_clear * common_clear).reshape(STATIONS, WINDOWS // 32, 32)
    shifts = jnp.arange(32, dtype=jnp.int32)
    return jnp.sum(jnp.left_shift(flag_grid, shifts[None, None, :]), axis=2).astype(jnp.int32)


def touch_ends(values, rng, smallest, high):
    extent = values.shape
    spot = [jax.random.randint(jax.random.fold_in(rng, axis), (), 0, extent[axis]) for axis in range(len(extent))]
    values = values.at[tuple(spot)].set(smallest)
    longest = extent.index(max(extent))
    spot[longest] = (spot[longest] + 1) % extent[longest]
    return values.at[tuple(spot)].set(high)


def setup_inputs(seed: int = 0) -> dict:
    splits = jax.random.split(jax.random.key(seed), 4)
    records = draw_records(jax.random.fold_in(splits[3], 71), 0)
    gap_flags = draw_gap_flags(jax.random.fold_in(splits[3], 71), 0)
    station_mask = touch_ends((jax.random.randint(splits[2], (STATIONS,), 0, 8) < 7).astype(jnp.int32), jax.random.fold_in(splits[2], 1), 0, 1)
    return {"records": records, "gap_flags": gap_flags, "station_mask": station_mask}


FLOOR = 0.25

def transform_table(length, bin_count):
    sample_ids = jnp.arange(length, dtype=jnp.int32)
    bin_ids = jnp.arange(bin_count, dtype=jnp.int32)
    phase_ids = bin_ids[:, None] * sample_ids[None, :] % length
    angles = phase_ids.astype(jnp.float32) * (2.0 * math.pi / length)
    window_taper = 0.5 - 0.5 * jnp.cos(sample_ids.astype(jnp.float32) * (2.0 * math.pi / length))
    factor = window_taper / math.sqrt(length)
    dft_table = jnp.concatenate([jnp.cos(angles) * factor, -jnp.sin(angles) * factor], axis=0)
    return dft_table.astype(jnp.bfloat16)

def unpack_flags(packed_words):
    shifts = jnp.arange(32, dtype=jnp.int32)
    bit_values = jnp.bitwise_and(jnp.right_shift(packed_words[:, :, None], shifts[None, None, :]), 1)
    return bit_values.reshape(packed_words.shape[0], packed_words.shape[1] * 32)

def whiten(records, band_bins):
    bin_count = band_bins + 4
    dft_table = transform_table(records.shape[-1], bin_count)
    spectrum = jnp.einsum('cl,swl->scw', dft_table.astype(jnp.float32), records.astype(jnp.float32), precision=lax.Precision.HIGHEST)
    real_part = spectrum[:, :bin_count]
    imag_part = spectrum[:, bin_count:]
    magnitude = jnp.sqrt(real_part * real_part + imag_part * imag_part)
    smooth = (magnitude[:, 0:band_bins] + magnitude[:, 1:band_bins + 1] + magnitude[:, 2:band_bins + 2] + magnitude[:, 3:band_bins + 3] + magnitude[:, 4:band_bins + 4]) / 5.0
    factor = 1.0 / jnp.maximum(smooth, FLOOR)
    whitened = jnp.stack([real_part[:, 2:band_bins + 2] * factor, imag_part[:, 2:band_bins + 2] * factor], axis=2)
    return whitened.astype(jnp.bfloat16)

def reference(records, gap_flags, station_mask):
    band_bins = BAND
    usable = unpack_flags(gap_flags) * station_mask[:, None]
    group_size = math.gcd(STATIONS, 64)
    grouped = records.reshape(STATIONS // group_size, group_size, WINDOWS, SAMPLES)
    whitened = lax.map(lambda inputs: whiten(inputs, band_bins), grouped)
    whitened = whitened.reshape(STATIONS, band_bins, 2, WINDOWS)
    flag_rows = usable.astype(jnp.bfloat16)
    masked = whitened * flag_rows[:, None, None, :]
    pair_counts = jnp.dot(flag_rows, flag_rows.T, preferred_element_type=jnp.float32)
    divisor = jnp.maximum(pair_counts, 1.0)

    def one_bin(bin_index):
        bin_plane = lax.dynamic_index_in_dim(masked, bin_index, 1, keepdims=False)
        direct = bin_plane.reshape(STATIONS, 2 * WINDOWS)
        turned = jnp.concatenate([bin_plane[:, 1], -bin_plane[:, 0]], axis=1)
        real_part = jnp.dot(direct, direct.T, preferred_element_type=jnp.float32)
        imag_part = jnp.dot(turned, direct.T, preferred_element_type=jnp.float32)
        return jnp.stack([real_part, imag_part]) / divisor
    return lax.map(one_bin, jnp.arange(band_bins, dtype=jnp.int32))
```

```python
import math

import jax
import jax.numpy as jnp
from jax import lax
from jax.experimental import pallas as pl
from jax.experimental.pallas import tpu as pltpu
from jax.sharding import PartitionSpec as P

FLOOR = 0.25
MESH = pl.DeviceIdType.MESH
Y = 4
PLANE = 32
STA = 64
ROWS = 256
UP = (("own", 1), ("own", 2), ("fwd", 2), ("own", 0), ("fwd", 1), ("own", 3))
DOWN = (("own", 3), ("own", 0), ("fwd", 3), ("own", 2), ("own", 1), ("fwd", 0))


def transform_table(length, bin_count):
    sample_ids = jnp.arange(length, dtype=jnp.int32)
    bin_ids = jnp.arange(bin_count, dtype=jnp.int32)
    phase_ids = bin_ids[:, None] * sample_ids[None, :] % length
    angles = phase_ids.astype(jnp.float32) * (2.0 * math.pi / length)
    window_taper = 0.5 - 0.5 * jnp.cos(sample_ids.astype(jnp.float32) * (2.0 * math.pi / length))
    factor = window_taper / math.sqrt(length)
    dft_table = jnp.concatenate([jnp.cos(angles) * factor, -jnp.sin(angles) * factor], axis=0)
    return dft_table.astype(jnp.bfloat16)


def unpack_flags(packed_words):
    shifts = jnp.arange(32, dtype=jnp.int32)
    bit_values = jnp.bitwise_and(
        jnp.right_shift(packed_words[:, :, None], shifts[None, None, :]), 1
    )
    return bit_values.reshape(packed_words.shape[0], packed_words.shape[1] * 32)


def whiten(records, band_bins, flags):
    bin_count = band_bins + 4
    dft_table = transform_table(records.shape[-1], bin_count)
    spectrum = jnp.einsum("cl,swl->scw", dft_table, records, preferred_element_type=jnp.float32)
    real_part = spectrum[:, :bin_count]
    imag_part = spectrum[:, bin_count:]
    magnitude = jnp.sqrt(real_part * real_part + imag_part * imag_part)
    smooth = (
        magnitude[:, 0:band_bins]
        + magnitude[:, 1 : band_bins + 1]
        + magnitude[:, 2 : band_bins + 2]
        + magnitude[:, 3 : band_bins + 3]
        + magnitude[:, 4 : band_bins + 4]
    ) / 5.0
    factor = flags[:, None, :] / jnp.maximum(smooth, FLOOR)
    whitened = jnp.concatenate(
        [real_part[:, 2 : band_bins + 2] * factor, imag_part[:, 2 : band_bins + 2] * factor], axis=2
    )
    return whitened.astype(jnp.bfloat16).transpose(1, 0, 2)


def exchange_kernel(
    spec_ref, word_ref, out_ref, words_ref,
    gathered, turned, block,
    plane_send, plane_recv, word_send, word_recv,
    up_send, up_recv, down_send, down_recv, far_send, far_recv, side_send, side_recv,
):
    tm = lax.axis_index("tm")
    freq = lax.axis_index("freq")
    y, zl = tm // 2, tm % 2
    mine = 2 * freq + zl

    def plane_peer(offset):
        other = (mine + offset) % PLANE
        return other, (2 * y + other % 2, other // 2)

    def ring_peer(offset):
        return (2 * ((y + offset) % Y) + zl, freq)

    barrier = pltpu.get_barrier_semaphore()
    for offset in range(1, PLANE):
        pl.semaphore_signal(barrier, inc=1, device_id=plane_peer(offset)[1], device_id_type=MESH)
    for offset in range(1, Y):
        pl.semaphore_signal(barrier, inc=1, device_id=ring_peer(offset), device_id_type=MESH)
    pl.semaphore_wait(barrier, PLANE - 1 + Y - 1)

    row_at = pl.multiple_of(freq * STA, STA)
    plane = []
    for offset in range(1, PLANE):
        other, device = plane_peer(offset)
        copy = pltpu.make_async_remote_copy(
            word_ref, words_ref.at[y, mine],
            word_send.at[offset], word_recv.at[offset], device_id=device, device_id_type=MESH)
        copy.start()
        plane.append(copy)
    for offset in range(1, PLANE):
        other, device = plane_peer(offset)
        copy = pltpu.make_async_remote_copy(
            spec_ref.at[other], gathered.at[y, zl, pl.ds(row_at, STA), :],
            plane_send.at[offset], plane_recv.at[offset], device_id=device, device_id_type=MESH)
        copy.start()
        plane.append(copy)
    gathered[y, zl, pl.ds(row_at, STA), :] = spec_ref[mine]
    words_ref[y, mine] = word_ref[...]
    for copy in plane:
        copy.wait()

    far = []
    for offset in range(1, Y):
        copy = pltpu.make_async_remote_copy(
            words_ref.at[y], words_ref.at[y],
            far_send.at[offset], far_recv.at[offset],
            device_id=ring_peer(offset), device_id_type=MESH)
        copy.start()
        far.append(copy)

    def piece(owner, shift):
        at = pl.multiple_of(((owner + shift) % Y) * ROWS, ROWS)
        return gathered.at[owner, :, pl.ds(at, ROWS), :]

    def ring_copy(plan, slot, step, send, recv):
        kind, shift = plan[slot]
        owner = y if kind == "own" else (y - step + Y) % Y
        ref = piece(owner, shift)
        return pltpu.make_async_remote_copy(
            ref, ref, send.at[slot], recv.at[slot],
            device_id=ring_peer(step % Y), device_id_type=MESH)

    ups = [ring_copy(UP, slot, 1, up_send, up_recv) for slot in range(6)]
    downs = [ring_copy(DOWN, slot, -1, down_send, down_recv) for slot in range(6)]

    def multiply(shift):
        at = pl.multiple_of(((y + shift) % Y) * ROWS, ROWS)
        right = jnp.concatenate(
            [gathered[owner, part, pl.ds(at, ROWS), :] for owner in range(Y) for part in range(2)], axis=1)
        both = lax.dot_general(turned[...], right, (((1,), (1,)), ((), ())),
                               preferred_element_type=jnp.float32)
        block[shift] = both.reshape(2, ROWS, ROWS)
        col = pl.multiple_of(((y + shift) % Y) * ROWS, ROWS)
        half = pl.multiple_of((1 - zl) * 128, 128)
        copy = pltpu.make_async_remote_copy(
            block.at[shift, :, pl.ds(half, 128), :],
            out_ref.at[zl, :, :, pl.ds(col, ROWS)],
            side_send.at[shift], side_recv.at[shift],
            device_id=(2 * y + 1 - zl, freq), device_id_type=MESH)
        copy.start()
        kept = pl.multiple_of(zl * 128, 128)
        out_ref[zl, :, :, pl.ds(col, ROWS)] = block[shift, :, pl.ds(kept, 128), :]
        return copy

    for slot in (0, 1):
        ups[slot].start()
        downs[slot].start()
    downs[0].wait_recv()
    downs[2].start()
    ups[0].wait_recv()
    ups[1].wait_recv()
    ups[2].start()
    downs[1].wait_recv()
    ups[3].start()
    downs[3].start()
    ups[4].start()
    downs[4].start()
    ups[5].start()
    downs[5].start()
    ups[2].wait_recv()
    downs[2].wait_recv()
    row = pl.multiple_of(y * ROWS, ROWS)
    for owner in range(Y):
        for part in range(2):
            left = gathered[owner, part, pl.ds(row, ROWS), :]
            lane = (2 * owner + part) * 256
            turned[0:ROWS, lane : lane + 256] = left
            turned[ROWS : 2 * ROWS, lane : lane + 256] = jnp.concatenate(
                [left[:, 128:], -left[:, :128]], axis=1)
    sides = [multiply(0), multiply(1)]
    ups[3].wait_recv()
    downs[3].wait_recv()
    ups[4].wait_recv()
    sides.append(multiply(3))
    downs[4].wait_recv()
    ups[5].wait_recv()
    downs[5].wait_recv()
    sides.append(multiply(2))
    for copy in far:
        copy.wait()
    for copy in ups + downs:
        copy.wait_send()
    for copy in sides:
        copy.wait()


def exchange(spectra, words):
    dma = pltpu.SemaphoreType.DMA
    vmem = pl.BlockSpec(memory_space=pltpu.VMEM)
    return pl.pallas_call(
        exchange_kernel,
        out_shape=(
            jax.ShapeDtypeStruct((2, 2, 128, 1024), jnp.float32),
            jax.ShapeDtypeStruct((Y, PLANE, 4, 128), jnp.int32),
        ),
        in_specs=[vmem, vmem],
        out_specs=(vmem, vmem),
        scratch_shapes=[
            pltpu.VMEM((Y, 2, 1024, 256), jnp.bfloat16),
            pltpu.VMEM((2 * ROWS, 2048), jnp.bfloat16),
            pltpu.VMEM((Y, 2, ROWS, ROWS), jnp.float32),
            dma((PLANE,)), dma((PLANE,)), dma((PLANE,)), dma((PLANE,)),
            dma((6,)), dma((6,)), dma((6,)), dma((6,)),
            dma((Y,)), dma((Y,)), dma((Y,)), dma((Y,)),
        ],
        compiler_params=pltpu.CompilerParams(
            collective_id=0, has_side_effects=True, vmem_limit_bytes=48 << 20),
    )(spectra, words)


def local(records, gap_flags, station_mask):
    kept_words = gap_flags * station_mask[:, None]
    here_flags = unpack_flags(kept_words).astype(jnp.float32)
    spectra = whiten(records, PLANE, here_flags)
    words = jnp.pad(kept_words.T, ((0, 0), (0, 128 - STA)))
    stacks, all_words = exchange(spectra, words)
    every = all_words[:, :, :, :STA].reshape(Y, 16, 2, 4, STA)
    every = every.transpose(1, 4, 0, 2, 3).reshape(1024, 32)
    every_flags = unpack_flags(every).astype(jnp.bfloat16)
    row_start = lax.axis_index("tm") * 128
    row_flags = lax.dynamic_slice_in_dim(every_flags, row_start, 128, 0)
    counts = jnp.dot(row_flags, every_flags.T, preferred_element_type=jnp.float32)
    return stacks / jnp.maximum(counts, 1.0)


def solution(mesh):
    placed = (P("freq", "tm", None), P("freq", "tm"), P("freq"))
    return jax.shard_map(
        local, mesh=mesh, in_specs=placed, out_specs=P("freq", None, "tm", None), check_vma=False
    )
```

```python
import math

import jax
import jax.numpy as jnp
import numpy as np
from jax import lax
from jax.experimental import pallas as pl
from jax.experimental.pallas import tpu as pltpu
from jax.sharding import PartitionSpec as P

FLOOR = 0.25
MESH = pl.DeviceIdType.MESH
Y = 4
PLANE = 32
STA = 64
CHUNKS = 4
PART = STA // CHUNKS
WIN = 128
LEN = 512
ROWS = 256
SIDE = 128
SLOTS = 40
NT = (((1,), (1,)), ((), ()))
TN = (((0,), (0,)), ((), ()))
QUARTERS = tuple(("q", q) for q in range(CHUNKS))
WHOLE = ("w", 0)
FIRST, SECOND = ("h", 0), ("h", 1)
UP = (
    [("own", 1, q) for q in QUARTERS]
    + [("own", 2, q) for q in QUARTERS]
    + [("fwd", 2, q) for q in QUARTERS]
    + [("own", 0, WHOLE), ("fwd", 1, WHOLE), ("own", 3, FIRST), ("own", 3, SECOND)]
)
DOWN = (
    [("own", 3, q) for q in QUARTERS]
    + [("own", 0, q) for q in QUARTERS]
    + [("fwd", 3, q) for q in QUARTERS]
    + [("own", 2, WHOLE), ("own", 1, FIRST), ("fwd", 0, FIRST), ("own", 1, SECOND), ("fwd", 0, SECOND)]
)


def transform_table():
    t = np.arange(LEN)
    taper = (0.5 - 0.5 * np.cos(2.0 * math.pi * t / LEN)) / math.sqrt(LEN)
    table = np.zeros((2, 5, 8, LEN))
    for v in range(5):
        for i in range(8):
            b = 5 * i + v
            if b < 36:
                angle = 2.0 * math.pi * ((b * t) % LEN) / LEN
                table[0, v, i] = np.cos(angle) * taper
                table[1, v, i] = -np.sin(angle) * taper
    return jnp.asarray(table.reshape(2 * SLOTS, LEN).astype(np.float32)).astype(jnp.bfloat16)


def kernel(
    rec_hbm, table_ref, flag_ref, word_ref, out_ref, inv_ref,
    rec, usable, stage_re, stage_im, spec, gathered, turned, block, ring_words, all_words, flat_words, bits,
    rec_sem, plane_send, plane_recv, wring_send, wring_recv, wplane_send, wplane_recv,
    up_send, up_recv, down_send, down_recv, side_send, side_recv,
):
    tm = lax.axis_index("tm")
    freq = lax.axis_index("freq")
    y, zl = tm // 2, tm % 2
    mine = 2 * freq + zl

    def plane_device(other):
        return (2 * y + other % 2, other // 2)

    def ring_device(offset):
        return (2 * ((y + offset) % Y) + zl, freq)

    loads = []
    for q in range(CHUNKS):
        copy = pltpu.make_async_copy(
            rec_hbm.at[pl.ds(PART * q, PART)], rec.at[pl.ds(PART * q, PART)], rec_sem.at[q])
        copy.start()
        loads.append(copy)

    barrier = pltpu.get_barrier_semaphore()

    def greet(offset, carry):
        pl.semaphore_signal(
            barrier, inc=1, device_id=plane_device((mine + offset) % PLANE), device_id_type=MESH)
        return carry

    lax.fori_loop(1, PLANE, greet, 0)
    for offset in range(1, Y):
        pl.semaphore_signal(barrier, inc=1, device_id=ring_device(offset), device_id_type=MESH)

    lane = lax.broadcasted_iota(jnp.int32, (STA, WIN), 1)
    words = flag_ref[...]
    spread = jnp.broadcast_to(words[:, 0:1], (STA, WIN))
    for j in range(1, 4):
        spread = jnp.where(lane >= 32 * j, jnp.broadcast_to(words[:, j : j + 1], (STA, WIN)), spread)
    usable[...] = (lax.shift_right_logical(spread, lane % 32) & 1).astype(jnp.float32)

    def transform(q):
        def pair(n, carry):
            first = PART * q + 2 * n
            both = rec[pl.ds(first, 2)].reshape(2 * WIN, LEN)
            spectrum = lax.dot_general(table_ref[...], both, NT, preferred_element_type=jnp.float32)
            for s in range(2):
                re = [spectrum[8 * v : 8 * v + 8, WIN * s : WIN * (s + 1)] for v in range(5)]
                im = [spectrum[SLOTS + 8 * v : SLOTS + 8 * v + 8, WIN * s : WIN * (s + 1)] for v in range(5)]
                m = [jnp.sqrt(a * a + b * b) for a, b in zip(re, im)]

                def above(x):
                    return pltpu.roll(x, 7, 0)

                def below(x):
                    return pltpu.roll(x, 1, 0)

                low, high = m[0] + m[1], m[3] + m[4]
                sums = [
                    low + m[2] + below(high),
                    low + m[2] + m[3] + below(m[4]),
                    low + m[2] + high,
                    m[1] + m[2] + high + above(m[0]),
                    m[2] + high + above(low),
                ]
                keep = jnp.broadcast_to(usable[pl.ds(first + s, 1), :], (8, WIN))
                for v in range(5):
                    factor = keep / jnp.maximum(sums[v] * 0.2, FLOOR)
                    at = pl.multiple_of((2 * n + s) * SLOTS + 8 * v, 8)
                    stage_re[pl.ds(at, 8), :] = re[v] * factor
                    stage_im[pl.ds(at, 8), :] = im[v] * factor
            return carry

        lax.fori_loop(0, PART // 2, pair, 0)
        for p in range(PLANE):
            i, v = (p + 2) // 5, (p + 2) % 5
            for half, stage in ((0, stage_re), (1, stage_im)):
                rows = stage[pl.ds(8 * v + i, PART, stride=SLOTS), :]
                spec[p, PART * q : PART * (q + 1), WIN * half : WIN * (half + 1)] = rows.astype(jnp.bfloat16)

    def plane_copy(q, sender, receiver):
        at = pl.ds(PART * q, PART)
        return pltpu.make_async_remote_copy(
            spec.at[receiver, at, :], gathered.at[y, sender % 2, sender // 2, at, :],
            plane_send.at[q, receiver], plane_recv.at[q, sender],
            device_id=plane_device(receiver), device_id_type=MESH)

    def send_plane(q):
        def one(offset, carry):
            plane_copy(q, mine, (mine + offset) % PLANE).start()
            return carry

        lax.fori_loop(1, PLANE, one, 0)
        gathered[y, zl, freq, PART * q : PART * (q + 1), :] = spec[mine, PART * q : PART * (q + 1), :]

    def from_plane(q, shift):
        def one(i, carry):
            sender = 8 * ((y + shift) % Y) + i

            @pl.when(sender != mine)
            def _():
                plane_copy(q, sender, (sender + 1) % PLANE).wait_recv()

            return carry

        lax.fori_loop(0, 8, one, 0)

    for q in range(CHUNKS):
        loads[q].wait()
        transform(q)
        if q == 0:
            pl.semaphore_wait(barrier, PLANE - 1 + Y - 1)
        send_plane(q)

    ring_words[y] = word_ref[...]
    word_ring = [
        pltpu.make_async_remote_copy(
            word_ref, ring_words.at[y], wring_send.at[offset], wring_recv.at[offset],
            device_id=ring_device(offset), device_id_type=MESH)
        for offset in range(1, Y)
    ]
    for copy in word_ring:
        copy.start()

    def message(entry, slot, step, send, recv):
        kind, shift, (how, n) = entry
        owner = y if kind == "own" else (y - step + Y) % Y
        group = 4 * ((owner + shift) % Y)
        if how == "q":
            ref = gathered.at[owner, :, pl.ds(group, 4), pl.ds(PART * n, PART), :]
        elif how == "h":
            ref = gathered.at[owner, :, pl.ds(group + 2 * n, 2), :, :]
        else:
            ref = gathered.at[owner, :, pl.ds(group, 4), :, :]
        return pltpu.make_async_remote_copy(
            ref, ref, send.at[slot], recv.at[slot],
            device_id=ring_device(step % Y), device_id_type=MESH)

    ups = [message(entry, slot, 1, up_send, up_recv) for slot, entry in enumerate(UP)]
    downs = [message(entry, slot, -1, down_send, down_recv) for slot, entry in enumerate(DOWN)]

    for q in range(CHUNKS):
        from_plane(q, 1)
        ups[q].start()
        from_plane(q, 3)
        downs[q].start()
        from_plane(q, 2)
        ups[4 + q].start()
        from_plane(q, 0)
        downs[4 + q].start()
        if q == 0:
            for copy in word_ring:
                copy.wait()

            def word_copy(sender, receiver):
                return pltpu.make_async_remote_copy(
                    ring_words, all_words.at[sender],
                    wplane_send.at[receiver], wplane_recv.at[sender],
                    device_id=plane_device(receiver), device_id_type=MESH)

            def send_words(offset, carry):
                word_copy(mine, (mine + offset) % PLANE).start()
                return carry

            lax.fori_loop(1, PLANE, send_words, 0)
            all_words[mine] = ring_words[...]

    for q in range(CHUNKS):
        ups[4 + q].wait_recv()
        ups[8 + q].start()
        downs[q].wait_recv()
        downs[8 + q].start()
    ups[12].start()
    downs[12].start()
    for q in range(CHUNKS):
        ups[q].wait_recv()
    ups[13].start()
    downs[13].start()
    for q in range(CHUNKS):
        downs[4 + q].wait_recv()
    downs[14].start()
    ups[14].start()
    downs[15].start()
    downs[16].start()
    ups[15].start()

    def words_here(offset, carry):
        sender = (mine + offset) % PLANE
        word_copy(sender, sender).wait_recv()
        return carry

    lax.fori_loop(1, PLANE, words_here, 0)
    lane2 = lax.broadcasted_iota(jnp.int32, (2, WIN), 1)
    for owner in range(Y):
        for part in range(2):
            base = 4 * (2 * owner + part)
            for g in range(8):
                a = all_words[4 * g + part, owner]
                b = all_words[4 * g + 2 + part, owner]
                flat_words[base : base + 2, WIN * g : WIN * (g + 1)] = jnp.where(
                    lane2 < 64, a, pltpu.roll(b, 64, 1))
                flat_words[base + 2 : base + 4, WIN * g : WIN * (g + 1)] = jnp.where(
                    lane2 < 64, pltpu.roll(a, 64, 1), b)
    shifts = lax.broadcasted_iota(jnp.int32, (32, 1024), 0)

    def unpack(n, carry):
        row = jnp.broadcast_to(flat_words[pl.ds(n, 1), :], (32, 1024))
        bit = (lax.shift_right_logical(row, shifts) & 1).astype(jnp.float32)
        bits[pl.ds(pl.multiple_of(32 * n, 32), 32), :] = bit.astype(jnp.bfloat16)
        return carry

    lax.fori_loop(0, 32, unpack, 0)
    here = bits[:, pl.ds(pl.multiple_of(tm * SIDE, SIDE), SIDE)]
    counts = lax.dot_general(here, bits[...], TN, preferred_element_type=jnp.float32)
    inv_ref[...] = 1.0 / jnp.maximum(counts, 1.0)

    def multiply(shift, half=None):
        base = (y + shift) % Y
        count = 4 if half is None else 2
        width = STA * count
        group = 4 * base + (0 if half is None else 2 * half)
        right = jnp.concatenate(
            [gathered[owner, part, pl.ds(group, count)].reshape(width, 2 * WIN)
             for owner in range(Y) for part in range(2)], axis=1)
        both = lax.dot_general(turned[...], right, NT, preferred_element_type=jnp.float32)
        at = 0 if not half else width
        slot = shift if half is None else shift + 2 * half
        block[shift, :, :, at : at + width] = both.reshape(2, ROWS, width)
        col = pl.multiple_of(group * STA, SIDE)
        away = pl.multiple_of((1 - zl) * SIDE, SIDE)
        copy = pltpu.make_async_remote_copy(
            block.at[shift, :, pl.ds(away, SIDE), at : at + width],
            out_ref.at[zl, :, :, pl.ds(col, width)],
            side_send.at[slot], side_recv.at[slot],
            device_id=(2 * y + 1 - zl, freq), device_id_type=MESH)
        copy.start()
        kept = pl.multiple_of(zl * SIDE, SIDE)
        out_ref[zl, :, :, pl.ds(col, width)] = block[shift, :, pl.ds(kept, SIDE), at : at + width]
        return copy

    for q in range(CHUNKS):
        ups[8 + q].wait_recv()
        downs[8 + q].wait_recv()
    for owner in range(Y):
        for part in range(2):
            left = gathered[owner, part, pl.ds(4 * y, 4)].reshape(ROWS, 2 * WIN)
            at = (2 * owner + part) * 256
            turned[0:ROWS, at : at + 256] = left
            turned[ROWS : 2 * ROWS, at : at + 256] = jnp.concatenate(
                [left[:, WIN:], -left[:, :WIN]], axis=1)
    sides = [multiply(0), multiply(1)]
    ups[12].wait_recv()
    downs[12].wait_recv()
    ups[13].wait_recv()
    sides.append(multiply(3))
    downs[13].wait_recv()
    downs[14].wait_recv()
    ups[14].wait_recv()
    sides.append(multiply(2, 0))
    downs[15].wait_recv()
    downs[16].wait_recv()
    ups[15].wait_recv()
    sides.append(multiply(2, 1))

    def sent(offset, carry):
        other = (mine + offset) % PLANE
        for q in range(CHUNKS):
            plane_copy(q, mine, other).wait_send()
        word_copy(mine, other).wait_send()
        return carry

    lax.fori_loop(1, PLANE, sent, 0)
    for copy in ups + downs:
        copy.wait_send()
    for copy in sides:
        copy.wait()


def stack_up(records, table, flags, words):
    dma = pltpu.SemaphoreType.DMA
    vmem = pl.BlockSpec(memory_space=pltpu.VMEM)
    return pl.pallas_call(
        kernel,
        out_shape=(
            jax.ShapeDtypeStruct((2, 2, SIDE, 1024), jnp.float32),
            jax.ShapeDtypeStruct((SIDE, 1024), jnp.float32),
        ),
        in_specs=[pl.BlockSpec(memory_space=pl.ANY), vmem, vmem, vmem],
        out_specs=(vmem, vmem),
        scratch_shapes=[
            pltpu.VMEM((STA, WIN, LEN), jnp.bfloat16),
            pltpu.VMEM((STA, WIN), jnp.float32),
            pltpu.VMEM((PART * SLOTS, WIN), jnp.float32),
            pltpu.VMEM((PART * SLOTS, WIN), jnp.float32),
            pltpu.VMEM((PLANE, STA, 2 * WIN), jnp.bfloat16),
            pltpu.VMEM((Y, 2, 16, STA, 2 * WIN), jnp.bfloat16),
            pltpu.VMEM((2 * ROWS, 2048), jnp.bfloat16),
            pltpu.VMEM((Y, 2, ROWS, ROWS), jnp.float32),
            pltpu.VMEM((Y, 2, WIN), jnp.int32),
            pltpu.VMEM((PLANE, Y, 2, WIN), jnp.int32),
            pltpu.VMEM((PLANE, 1024), jnp.int32),
            pltpu.VMEM((1024, 1024), jnp.bfloat16),
            dma((CHUNKS,)), dma((CHUNKS, PLANE)), dma((CHUNKS, PLANE)),
            dma((Y,)), dma((Y,)), dma((PLANE,)), dma((PLANE,)),
            dma((len(UP),)), dma((len(UP),)), dma((len(DOWN),)), dma((len(DOWN),)),
            dma((5,)), dma((5,)),
        ],
        compiler_params=pltpu.CompilerParams(
            collective_id=0, has_side_effects=True, vmem_limit_bytes=56 << 20),
    )(records, table, flags, words)


def local(records, gap_flags, station_mask):
    kept = gap_flags * station_mask[:, None]
    words = kept.T.reshape(2, WIN)
    stacks, inverse = stack_up(records, transform_table(), kept, words)
    return stacks * inverse


def solution(mesh):
    placed = (P("freq", "tm", None), P("freq", "tm"), P("freq"))
    return jax.shard_map(
        local, mesh=mesh, in_specs=placed, out_specs=P("freq", None, "tm", None), check_vma=False
    )
```

```python
import math

import jax
import jax.numpy as jnp
import numpy as np
from jax import lax
from jax.experimental import pallas as pl
from jax.experimental.pallas import tpu as pltpu
from jax.sharding import PartitionSpec as P

FLOOR = 0.25
MESH = pl.DeviceIdType.MESH
Y = 4
PLANE = 32
STA = 64
CHUNKS = 4
PART = STA // CHUNKS
WIN = 128
LEN = 512
ROWS = 256
SIDE = 128
STEP = 4
SLOTS = 40
NT = (((1,), (1,)), ((), ()))
TN = (((0,), (0,)), ((), ()))
QUARTERS = tuple(("q", q) for q in range(CHUNKS))
FIRST, SECOND = ("h", 0), ("h", 1)
UP = (
    [("own", 1, q) for q in QUARTERS]
    + [("own", 2, q) for q in QUARTERS]
    + [("fwd", 2, q) for q in QUARTERS]
    + [("own", 3, FIRST), ("own", 3, SECOND)]
)
DOWN = (
    [("own", 3, q) for q in QUARTERS]
    + [("own", 0, q) for q in QUARTERS]
    + [("fwd", 3, q) for q in QUARTERS]
    + [("own", 1, FIRST), ("fwd", 0, FIRST), ("own", 1, SECOND), ("fwd", 0, SECOND)]
)


def transform_table():
    t = np.arange(LEN)
    taper = (0.5 - 0.5 * np.cos(2.0 * math.pi * t / LEN)) / math.sqrt(LEN)
    table = np.zeros((2, 5, 8, LEN))
    for v in range(5):
        for i in range(8):
            b = 5 * i + v
            if b < 36:
                angle = 2.0 * math.pi * ((b * t) % LEN) / LEN
                table[0, v, i] = np.cos(angle) * taper
                table[1, v, i] = -np.sin(angle) * taper
    return jnp.asarray(table.reshape(2 * SLOTS, LEN).astype(np.float32)).astype(jnp.bfloat16)


def kernel(
    rec_hbm, table_ref, flag_ref, mask_ref, out_ref,
    rec, kept, square, word_ref, usable, stage_re, stage_im, spec, gathered, turned, block,
    ring_words, all_words, flat_words, bits, inverse, side_out, side_in, mirror_out, mirror_in,
    side_scale_out, side_scale_in, mirror_scale_out, mirror_scale_in,
    rec_sem, plane_send, plane_recv, wring_send, wring_recv, wplane_send, wplane_recv,
    up_send, up_recv, down_send, down_recv, side_send, side_recv, mirror_send, mirror_recv,
):
    tm = lax.axis_index("tm")
    freq = lax.axis_index("freq")
    y, zl = tm // 2, tm % 2
    mine = 2 * freq + zl

    def plane_device(other):
        return (2 * y + other % 2, other // 2)

    def ring_device(offset):
        return (2 * ((y + offset) % Y) + zl, freq)

    def cross_device(offset):
        return (2 * ((y + offset) % Y) + 1 - zl, freq)

    loads = []
    for q in range(CHUNKS):
        copy = pltpu.make_async_copy(
            rec_hbm.at[pl.ds(PART * q, PART)], rec.at[pl.ds(PART * q, PART)], rec_sem.at[q])
        copy.start()
        loads.append(copy)

    barrier = pltpu.get_barrier_semaphore()

    def greet(offset, carry):
        pl.semaphore_signal(
            barrier, inc=1, device_id=plane_device((mine + offset) % PLANE), device_id_type=MESH)
        return carry

    lax.fori_loop(1, PLANE, greet, 0)
    for offset in range(1, Y):
        pl.semaphore_signal(barrier, inc=1, device_id=ring_device(offset), device_id_type=MESH)
    for offset in (1, Y - 1):
        pl.semaphore_signal(barrier, inc=1, device_id=cross_device(offset), device_id_type=MESH)

    kept[...] = jnp.zeros_like(kept)
    kept[0:4, 0:STA] = flag_ref[...] * mask_ref[...]
    square[...] = jnp.zeros_like(square)
    square[0:8, :] = kept[...]
    words = jnp.transpose(square[...])[0:STA]
    lane = lax.broadcasted_iota(jnp.int32, (STA, WIN), 1)
    spread = jnp.broadcast_to(words[:, 0:1], (STA, WIN))
    for j in range(1, 4):
        spread = jnp.where(lane >= 32 * j, jnp.broadcast_to(words[:, j : j + 1], (STA, WIN)), spread)
    usable[...] = (lax.shift_right_logical(spread, lane % 32) & 1).astype(jnp.float32)
    low = lax.broadcasted_iota(jnp.int32, (1, WIN), 1) < STA
    rows = kept[...]
    rolled = pltpu.roll(rows, STA, 1)
    word_ref[0:1] = jnp.where(low, rows[0:1], rolled[1:2])
    word_ref[1:2] = jnp.where(low, rows[2:3], rolled[3:4])

    def transform(q):
        def pair(n, carry):
            first = PART * q + STEP * n
            both = rec[pl.ds(first, STEP)].reshape(STEP * WIN, LEN)
            spectrum = lax.dot_general(table_ref[...], both, NT, preferred_element_type=jnp.float32)
            for s in range(STEP):
                re = [spectrum[8 * v : 8 * v + 8, WIN * s : WIN * (s + 1)] for v in range(5)]
                im = [spectrum[SLOTS + 8 * v : SLOTS + 8 * v + 8, WIN * s : WIN * (s + 1)] for v in range(5)]
                m = [jnp.sqrt(a * a + b * b) for a, b in zip(re, im)]

                def above(x):
                    return pltpu.roll(x, 7, 0)

                def below(x):
                    return pltpu.roll(x, 1, 0)

                low, high = m[0] + m[1], m[3] + m[4]
                sums = [
                    low + m[2] + below(high),
                    low + m[2] + m[3] + below(m[4]),
                    low + m[2] + high,
                    m[1] + m[2] + high + above(m[0]),
                    m[2] + high + above(low),
                ]
                keep = jnp.broadcast_to(usable[pl.ds(first + s, 1), :], (8, WIN))
                for v in range(5):
                    factor = keep / jnp.maximum(sums[v] * 0.2, FLOOR)
                    at = pl.multiple_of((STEP * n + s) * SLOTS + 8 * v, 8)
                    stage_re[pl.ds(at, 8), :] = re[v] * factor
                    stage_im[pl.ds(at, 8), :] = im[v] * factor
            return carry

        lax.fori_loop(0, PART // STEP, pair, 0)
        for p in range(PLANE):
            i, v = (p + 2) // 5, (p + 2) % 5
            for half, stage in ((0, stage_re), (1, stage_im)):
                rows = stage[pl.ds(8 * v + i, PART, stride=SLOTS), :]
                spec[p, PART * q : PART * (q + 1), WIN * half : WIN * (half + 1)] = rows.astype(jnp.bfloat16)

    def plane_copy(q, sender, receiver):
        at = pl.ds(PART * q, PART)
        return pltpu.make_async_remote_copy(
            spec.at[receiver, at, :], gathered.at[y, sender % 2, sender // 2, at, :],
            plane_send.at[q, receiver], plane_recv.at[q, sender],
            device_id=plane_device(receiver), device_id_type=MESH)

    def send_plane(q):
        def one(offset, carry):
            plane_copy(q, mine, (mine + offset) % PLANE).start()
            return carry

        lax.fori_loop(1, PLANE, one, 0)
        gathered[y, zl, freq, PART * q : PART * (q + 1), :] = spec[mine, PART * q : PART * (q + 1), :]

    def from_plane(q, shift):
        def one(i, carry):
            sender = 8 * ((y + shift) % Y) + i

            @pl.when(sender != mine)
            def _():
                plane_copy(q, sender, (sender + 1) % PLANE).wait_recv()

            return carry

        lax.fori_loop(0, 8, one, 0)

    for q in range(CHUNKS):
        loads[q].wait()
        transform(q)
        if q == 0:
            pl.semaphore_wait(barrier, PLANE - 1 + Y - 1 + 2)
        send_plane(q)

    ring_words[y] = word_ref[...]
    word_ring = [
        pltpu.make_async_remote_copy(
            word_ref, ring_words.at[y], wring_send.at[offset], wring_recv.at[offset],
            device_id=ring_device(offset), device_id_type=MESH)
        for offset in range(1, Y)
    ]
    for copy in word_ring:
        copy.start()

    def message(entry, slot, step, send, recv):
        kind, shift, (how, n) = entry
        owner = y if kind == "own" else (y - step + Y) % Y
        group = 4 * ((owner + shift) % Y)
        if how == "q":
            ref = gathered.at[owner, :, pl.ds(group, 4), pl.ds(PART * n, PART), :]
        else:
            ref = gathered.at[owner, :, pl.ds(group + 2 * n, 2), :, :]
        return pltpu.make_async_remote_copy(
            ref, ref, send.at[slot], recv.at[slot],
            device_id=ring_device(step % Y), device_id_type=MESH)

    ups = [message(entry, slot, 1, up_send, up_recv) for slot, entry in enumerate(UP)]
    downs = [message(entry, slot, -1, down_send, down_recv) for slot, entry in enumerate(DOWN)]

    for q in range(CHUNKS):
        from_plane(q, 1)
        ups[q].start()
        from_plane(q, 3)
        downs[q].start()
        from_plane(q, 2)
        ups[4 + q].start()
        from_plane(q, 0)
        downs[4 + q].start()
        if q == 0:
            for copy in word_ring:
                copy.wait()

            def word_copy(sender, receiver):
                return pltpu.make_async_remote_copy(
                    ring_words, all_words.at[sender],
                    wplane_send.at[receiver], wplane_recv.at[sender],
                    device_id=plane_device(receiver), device_id_type=MESH)

            def send_words(offset, carry):
                word_copy(mine, (mine + offset) % PLANE).start()
                return carry

            lax.fori_loop(1, PLANE, send_words, 0)
            all_words[mine] = ring_words[...]

    for q in range(CHUNKS):
        ups[4 + q].wait_recv()
        ups[8 + q].start()
        downs[q].wait_recv()
        downs[8 + q].start()
    ups[12].start()
    downs[12].start()
    for q in range(CHUNKS):
        downs[4 + q].wait_recv()
    downs[13].start()
    downs[14].start()
    downs[15].start()

    def words_here(offset, carry):
        sender = (mine + offset) % PLANE
        word_copy(sender, sender).wait_recv()
        return carry

    lax.fori_loop(1, PLANE, words_here, 0)
    lane2 = lax.broadcasted_iota(jnp.int32, (2, WIN), 1)
    for owner in range(Y):
        for part in range(2):
            base = 4 * (2 * owner + part)
            for g in range(8):
                a = all_words[4 * g + part, owner]
                b = all_words[4 * g + 2 + part, owner]
                flat_words[base : base + 2, WIN * g : WIN * (g + 1)] = jnp.where(
                    lane2 < 64, a, pltpu.roll(b, 64, 1))
                flat_words[base + 2 : base + 4, WIN * g : WIN * (g + 1)] = jnp.where(
                    lane2 < 64, pltpu.roll(a, 64, 1), b)
    shifts = lax.broadcasted_iota(jnp.int32, (32, 1024), 0)

    def unpack(n, carry):
        row = jnp.broadcast_to(flat_words[pl.ds(n, 1), :], (32, 1024))
        bit = (lax.shift_right_logical(row, shifts) & 1).astype(jnp.float32)
        bits[pl.ds(pl.multiple_of(32 * n, 32), 32), :] = bit.astype(jnp.bfloat16)
        return carry

    lax.fori_loop(0, 32, unpack, 0)
    here = bits[:, pl.ds(pl.multiple_of(y * ROWS, ROWS), ROWS)]
    counts = lax.dot_general(here, bits[...], TN, preferred_element_type=jnp.float32)
    inverse[...] = 1.0 / jnp.maximum(counts, 1.0)
    kept_at = pl.multiple_of(zl * SIDE, SIDE)
    away_at = pl.multiple_of((1 - zl) * SIDE, SIDE)

    def encode(values):
        top = jnp.maximum(jnp.max(jnp.abs(values), axis=0, keepdims=True), 1e-30)
        codes = jnp.round(values * (32767.0 / top)).astype(jnp.int32).astype(jnp.int16)
        return codes, top / 32767.0

    def decode(codes, scale):
        return codes.astype(jnp.int32).astype(jnp.float32) * scale

    def multiply(shift, half=None):
        count = 4 if half is None else 2
        width = STA * count
        group = 4 * ((y + shift) % Y) + (0 if half is None else 2 * half)
        right = jnp.concatenate(
            [gathered[owner, part, pl.ds(group, count)].reshape(width, 2 * WIN)
             for owner in range(Y) for part in range(2)], axis=1)
        both = lax.dot_general(turned[...], right, NT, preferred_element_type=jnp.float32)
        at = slice(SIDE, ROWS) if half == 1 else slice(0, width)
        slot = shift if half is None else shift + half
        col = pl.multiple_of(group * STA, SIDE)
        scale = inverse[:, pl.ds(col, width)]
        block[shift, :, :, at] = both.reshape(2, ROWS, width) * scale
        for plane in range(2):
            side_out[shift, plane, :, at], side_scale_out[slot, plane : plane + 1, 0:width] = encode(
                block[shift, plane, pl.ds(away_at, SIDE), at])
        copies = [
            pltpu.make_async_remote_copy(
                source, target, side_send.at[kind, slot], side_recv.at[kind, slot],
                device_id=(2 * y + 1 - zl, freq), device_id_type=MESH)
            for kind, (source, target) in enumerate((
                (side_scale_out.at[slot], side_scale_in.at[slot]),
                (side_out.at[shift, :, :, at], side_in.at[shift, :, :, at])))
        ]
        for copy in copies:
            copy.start()
        out_ref[zl, :, :, pl.ds(col, width)] = block[shift, :, pl.ds(kept_at, SIDE), at]
        return copies

    for q in range(CHUNKS):
        ups[q].wait_recv()
        ups[8 + q].wait_recv()
        downs[8 + q].wait_recv()
    for owner in range(Y):
        for part in range(2):
            left = gathered[owner, part, pl.ds(4 * y, 4)].reshape(ROWS, 2 * WIN)
            at = (2 * owner + part) * 256
            turned[0:ROWS, at : at + 256] = left
            turned[ROWS : 2 * ROWS, at : at + 256] = jnp.concatenate(
                [left[:, WIN:], -left[:, :WIN]], axis=1)
    sides = [multiply(1)]
    for plane, sign in ((0, 1.0), (1, -1.0)):
        flipped = sign * jnp.transpose(block[1, plane])
        for h in range(2):
            mirror_out[h, plane], mirror_scale_out[h, plane : plane + 1] = encode(
                flipped[SIDE * h : SIDE * (h + 1)])
    mirrors = [
        pltpu.make_async_remote_copy(
            source.at[part], target.at[zl],
            mirror_send.at[kind, n], mirror_recv.at[kind, n], device_id=device, device_id_type=MESH)
        for n, (part, device) in enumerate(((zl, ring_device(1)), (1 - zl, cross_device(1))))
        for kind, (source, target) in enumerate(
            ((mirror_scale_out, mirror_scale_in), (mirror_out, mirror_in)))
    ]
    for copy in mirrors:
        copy.start()
    ups[13].start()
    sides.append(multiply(0))
    ups[12].wait_recv()
    downs[12].wait_recv()
    downs[13].wait_recv()
    sides.append(multiply(2, 0))
    ups[13].wait_recv()
    downs[14].wait_recv()
    downs[15].wait_recv()
    sides.append(multiply(2, 1))

    def sent(offset, carry):
        other = (mine + offset) % PLANE
        for q in range(CHUNKS):
            plane_copy(q, mine, other).wait_send()
        word_copy(mine, other).wait_send()
        return carry

    lax.fori_loop(1, PLANE, sent, 0)
    for copy in ups + downs:
        copy.wait_send()

    def column(shift):
        return pl.ds(pl.multiple_of(((y + shift) % Y) * ROWS, ROWS), ROWS)

    for shift in (1, 0):
        for copy in sides[1 - shift]:
            copy.wait()
        for plane in range(2):
            out_ref[1 - zl, plane, :, column(shift)] = decode(
                side_in[shift, plane], side_scale_in[shift, plane : plane + 1])
    for copy in mirrors:
        copy.wait()
    for n in range(2):
        for plane in range(2):
            out_ref[n, plane, :, column(3)] = decode(
                mirror_in[n, plane], mirror_scale_in[n, plane : plane + 1])
    for half in range(2):
        for copy in sides[2 + half]:
            copy.wait()
        at = slice(SIDE * half, SIDE * (half + 1))
        col = pl.multiple_of(((y + 2) % Y) * ROWS + SIDE * half, SIDE)
        for plane in range(2):
            out_ref[1 - zl, plane, :, pl.ds(col, SIDE)] = decode(
                side_in[2, plane, :, at], side_scale_in[2 + half, plane : plane + 1, 0:SIDE])


def stack_up(records, table, flags, mask):
    dma = pltpu.SemaphoreType.DMA
    vmem = pl.BlockSpec(memory_space=pltpu.VMEM)
    return pl.pallas_call(
        kernel,
        out_shape=jax.ShapeDtypeStruct((2, 2, SIDE, 1024), jnp.float32),
        in_specs=[pl.BlockSpec(memory_space=pltpu.HBM), vmem, vmem, vmem],
        out_specs=vmem,
        scratch_shapes=[
            pltpu.VMEM((STA, WIN, LEN), jnp.bfloat16),
            pltpu.VMEM((8, WIN), jnp.int32),
            pltpu.VMEM((WIN, WIN), jnp.int32),
            pltpu.VMEM((2, WIN), jnp.int32),
            pltpu.VMEM((STA, WIN), jnp.float32),
            pltpu.VMEM((PART * SLOTS, WIN), jnp.float32),
            pltpu.VMEM((PART * SLOTS, WIN), jnp.float32),
            pltpu.VMEM((PLANE, STA, 2 * WIN), jnp.bfloat16),
            pltpu.VMEM((Y, 2, 16, STA, 2 * WIN), jnp.bfloat16),
            pltpu.VMEM((2 * ROWS, 2048), jnp.bfloat16),
            pltpu.VMEM((3, 2, ROWS, ROWS), jnp.float32),
            pltpu.VMEM((Y, 2, WIN), jnp.int32),
            pltpu.VMEM((PLANE, Y, 2, WIN), jnp.int32),
            pltpu.VMEM((PLANE, 1024), jnp.int32),
            pltpu.VMEM((1024, 1024), jnp.bfloat16),
            pltpu.VMEM((ROWS, 1024), jnp.float32),
            pltpu.VMEM((3, 2, SIDE, ROWS), jnp.int16),
            pltpu.VMEM((3, 2, SIDE, ROWS), jnp.int16),
            pltpu.VMEM((2, 2, SIDE, ROWS), jnp.int16),
            pltpu.VMEM((2, 2, SIDE, ROWS), jnp.int16),
            pltpu.VMEM((4, 2, ROWS), jnp.float32),
            pltpu.VMEM((4, 2, ROWS), jnp.float32),
            pltpu.VMEM((2, 2, ROWS), jnp.float32),
            pltpu.VMEM((2, 2, ROWS), jnp.float32),
            dma((CHUNKS,)), dma((CHUNKS, PLANE)), dma((CHUNKS, PLANE)),
            dma((Y,)), dma((Y,)), dma((PLANE,)), dma((PLANE,)),
            dma((len(UP),)), dma((len(UP),)), dma((len(DOWN),)), dma((len(DOWN),)),
            dma((2, 4)), dma((2, 4)), dma((2, 2)), dma((2, 2)),
        ],
        compiler_params=pltpu.CompilerParams(
            collective_id=0, has_side_effects=True, vmem_limit_bytes=48 << 20),
    )(records, table, flags, mask)


def local(records, gap_flags, station_mask):
    return stack_up(records, transform_table(), gap_flags.T, station_mask[None])


def solution(mesh):
    placed = (P("freq", "tm", None), P("freq", "tm"), P("freq"))
    return jax.shard_map(
        local, mesh=mesh, in_specs=placed, out_specs=P("freq", None, "tm", None), check_vma=False
    )
```

```python
import math

import jax
import jax.numpy as jnp
import numpy as np
from jax import lax
from jax.experimental import pallas as pl
from jax.experimental.pallas import tpu as pltpu
from jax.sharding import PartitionSpec as P

FLOOR = 0.25
MESH = pl.DeviceIdType.MESH
Y = 4
PLANE = 32
STA = 64
CHUNKS = 4
PART = STA // CHUNKS
WIN = 128
LEN = 512
ROWS = 256
SIDE = 128
STEP = 8
SLOTS = 40
NEAR = (0, 1, 3, 2)
OWNERS = (0, 1, 3, 2)
NT = (((1,), (1,)), ((), ()))
TN = (((0,), (0,)), ((), ()))
QUARTERS = tuple(("q", q) for q in range(CHUNKS))
FIRST, SECOND = ("h", 0), ("h", 1)
UP = (
    [("own", 1, q) for q in QUARTERS]
    + [("own", 2, q) for q in QUARTERS]
    + [("fwd", 2, q) for q in QUARTERS]
    + [("own", 3, FIRST), ("own", 3, SECOND)]
)
DOWN = (
    [("own", 3, q) for q in QUARTERS]
    + [("own", 0, q) for q in QUARTERS]
    + [("fwd", 3, q) for q in QUARTERS]
    + [("own", 1, FIRST), ("fwd", 0, FIRST), ("own", 1, SECOND), ("fwd", 0, SECOND)]
)


def transform_table():
    t = np.arange(LEN)
    taper = (0.5 - 0.5 * np.cos(2.0 * math.pi * t / LEN)) / math.sqrt(LEN)
    table = np.zeros((2, 5, 8, LEN))
    for v in range(5):
        for i in range(8):
            b = 5 * i + v
            if b < 36:
                angle = 2.0 * math.pi * ((b * t) % LEN) / LEN
                table[0, v, i] = np.cos(angle) * taper
                table[1, v, i] = -np.sin(angle) * taper
    return jnp.asarray(table.reshape(2 * SLOTS, LEN).astype(np.float32)).astype(jnp.bfloat16)


def kernel(
    rec_hbm, table_hbm, flag_hbm, mask_hbm, out_hbm,
    rec, table_ref, flag_ref, mask_ref, out_ref, kept, square, word_ref, usable, stage_re, stage_im, spec, gathered, turned, block,
    ring_words, all_words, flat_words, bits, inverse, side_out, side_in, mirror_out, mirror_in,
    side_scale_out, side_scale_in, mirror_scale_out, mirror_scale_in,
    rec_sem, small_sem, out_sem, plane_send, plane_recv, wring_send, wring_recv, wplane_send, wplane_recv,
    up_send, up_recv, down_send, down_recv, side_send, side_recv, mirror_send, mirror_recv,
):
    tm = lax.axis_index("tm")
    freq = lax.axis_index("freq")
    y, zl = tm // 2, tm % 2
    mine = 2 * freq + zl
    x, spot = mine // 8, mine % 8

    def plane_device(other):
        return (2 * y + other % 2, other // 2)

    def ring_device(offset):
        return (2 * ((y + offset) % Y) + zl, freq)

    def cross_device(offset):
        return (2 * ((y + offset) % Y) + 1 - zl, freq)

    small = [
        pltpu.make_async_copy(source, target, small_sem.at[n])
        for n, (source, target) in enumerate(
            ((flag_hbm, flag_ref), (mask_hbm, mask_ref), (table_hbm, table_ref)))
    ]
    loads = [
        pltpu.make_async_copy(
            rec_hbm.at[pl.ds(PART * q, PART)], rec.at[pl.ds(PART * q, PART)], rec_sem.at[q])
        for q in range(CHUNKS)
    ]
    for copy in small:
        copy.start()
    loads[0].start()

    barrier = pltpu.get_barrier_semaphore()

    def greet(offset, carry):
        pl.semaphore_signal(
            barrier, inc=1, device_id=plane_device((mine + offset) % PLANE), device_id_type=MESH)
        return carry

    lax.fori_loop(1, PLANE, greet, 0)
    for offset in range(1, Y):
        pl.semaphore_signal(barrier, inc=1, device_id=ring_device(offset), device_id_type=MESH)
    for offset in (1, Y - 1):
        pl.semaphore_signal(barrier, inc=1, device_id=cross_device(offset), device_id_type=MESH)

    for copy in small:
        copy.wait()
    kept[...] = jnp.zeros_like(kept)
    kept[0:4, 0:STA] = flag_ref[...] * mask_ref[...]
    square[...] = jnp.zeros_like(square)
    square[0:8, :] = kept[...]
    words = jnp.transpose(square[...])[0:STA]
    lane = lax.broadcasted_iota(jnp.int32, (STA, WIN), 1)
    spread = jnp.broadcast_to(words[:, 0:1], (STA, WIN))
    for j in range(1, 4):
        spread = jnp.where(lane >= 32 * j, jnp.broadcast_to(words[:, j : j + 1], (STA, WIN)), spread)
    usable[...] = (lax.shift_right_logical(spread, lane % 32) & 1).astype(jnp.float32)
    low = lax.broadcasted_iota(jnp.int32, (1, WIN), 1) < STA
    rows = kept[...]
    rolled = pltpu.roll(rows, STA, 1)
    word_ref[0:1] = jnp.where(low, rows[0:1], rolled[1:2])
    word_ref[1:2] = jnp.where(low, rows[2:3], rolled[3:4])

    def transform(q):
        def pair(n, carry):
            first = PART * q + STEP * n
            both = rec[pl.ds(first, STEP)].reshape(STEP * WIN, LEN)
            spectrum = lax.dot_general(table_ref[...], both, NT, preferred_element_type=jnp.float32)
            for s in range(STEP):
                re = [spectrum[8 * v : 8 * v + 8, WIN * s : WIN * (s + 1)] for v in range(5)]
                im = [spectrum[SLOTS + 8 * v : SLOTS + 8 * v + 8, WIN * s : WIN * (s + 1)] for v in range(5)]
                m = [jnp.sqrt(a * a + b * b) for a, b in zip(re, im)]

                def above(x):
                    return pltpu.roll(x, 7, 0)

                def below(x):
                    return pltpu.roll(x, 1, 0)

                low, high = m[0] + m[1], m[3] + m[4]
                sums = [
                    low + m[2] + below(high),
                    low + m[2] + m[3] + below(m[4]),
                    low + m[2] + high,
                    m[1] + m[2] + high + above(m[0]),
                    m[2] + high + above(low),
                ]
                keep = jnp.broadcast_to(usable[pl.ds(first + s, 1), :], (8, WIN))
                for v in range(5):
                    factor = keep / jnp.maximum(sums[v] * 0.2, FLOOR)
                    at = pl.multiple_of((STEP * n + s) * SLOTS + 8 * v, 8)
                    stage_re[pl.ds(at, 8), :] = re[v] * factor
                    stage_im[pl.ds(at, 8), :] = im[v] * factor
            return carry

        lax.fori_loop(0, PART // STEP, pair, 0)
        for p in range(PLANE):
            i, v = (p + 2) // 5, (p + 2) % 5
            for half, stage in ((0, stage_re), (1, stage_im)):
                rows = stage[pl.ds(8 * v + i, PART, stride=SLOTS), :]
                spec[p, PART * q : PART * (q + 1), WIN * half : WIN * (half + 1)] = rows.astype(jnp.bfloat16)

    def plane_copy(q, sender, receiver):
        at = pl.ds(PART * q, PART)
        return pltpu.make_async_remote_copy(
            spec.at[receiver, at, :], gathered.at[y, sender % 2, sender // 2, at, :],
            plane_send.at[q, receiver], plane_recv.at[q, sender],
            device_id=plane_device(receiver), device_id_type=MESH)

    def group_peer(step, j):
        return 8 * ((x + step) % 4) + (spot + j) % 8

    def send_plane(q):
        for step in NEAR:
            def one(j, carry):
                plane_copy(q, mine, group_peer(step, j)).start()
                return carry

            lax.fori_loop(0 if step else 1, 8, one, 0)
        gathered[y, zl, freq, PART * q : PART * (q + 1), :] = spec[mine, PART * q : PART * (q + 1), :]

    def from_plane(q, step):
        def one(j, carry):
            sender = group_peer(step, j)
            plane_copy(q, sender, (sender + 1) % PLANE).wait_recv()
            return carry

        lax.fori_loop(0 if step else 1, 8, one, 0)

    for q in range(CHUNKS):
        loads[q].wait()
        if q == 0:
            for copy in loads[1:]:
                copy.start()
        transform(q)
        if q == 0:
            pl.semaphore_wait(barrier, PLANE - 1 + Y - 1 + 2)
        send_plane(q)

    ring_words[y] = word_ref[...]
    word_ring = [
        pltpu.make_async_remote_copy(
            word_ref, ring_words.at[y], wring_send.at[offset], wring_recv.at[offset],
            device_id=ring_device(offset), device_id_type=MESH)
        for offset in range(1, Y)
    ]
    for copy in word_ring:
        copy.start()

    def message(entry, slot, step, send, recv):
        kind, shift, (how, n) = entry
        owner = y if kind == "own" else (y - step + Y) % Y
        group = 4 * ((owner + shift) % Y)
        if how == "q":
            ref = gathered.at[owner, :, pl.ds(group, 4), pl.ds(PART * n, PART), :]
        else:
            ref = gathered.at[owner, :, pl.ds(group + 2 * n, 2), :, :]
        return pltpu.make_async_remote_copy(
            ref, ref, send.at[slot], recv.at[slot],
            device_id=ring_device(step % Y), device_id_type=MESH)

    ups = [message(entry, slot, 1, up_send, up_recv) for slot, entry in enumerate(UP)]
    downs = [message(entry, slot, -1, down_send, down_recv) for slot, entry in enumerate(DOWN)]

    def ring_start(q, step):
        group = (x + step) % 4
        shift = (group - y + Y) % Y
        ref = gathered.at[y, :, pl.ds(4 * group, 4), pl.ds(PART * q, PART), :]
        upward = (shift + 1) // 2 == 1

        @pl.when(upward)
        def _():
            slot = CHUNKS * (shift - 1) + q
            pltpu.make_async_remote_copy(
                ref, ref, up_send.at[slot], up_recv.at[slot],
                device_id=ring_device(1), device_id_type=MESH).start()

        @pl.when(jnp.logical_not(upward))
        def _():
            slot = CHUNKS * ((3 - shift) // 3) + q
            pltpu.make_async_remote_copy(
                ref, ref, down_send.at[slot], down_recv.at[slot],
                device_id=ring_device(Y - 1), device_id_type=MESH).start()

    for q in range(CHUNKS):
        for step in NEAR:
            from_plane(q, step)
            ring_start(q, step)
        if q == 0:
            for copy in word_ring:
                copy.wait()

            def word_copy(sender, receiver):
                return pltpu.make_async_remote_copy(
                    ring_words, all_words.at[sender],
                    wplane_send.at[receiver], wplane_recv.at[sender],
                    device_id=plane_device(receiver), device_id_type=MESH)

            def send_words(offset, carry):
                word_copy(mine, (mine + offset) % PLANE).start()
                return carry

            lax.fori_loop(1, PLANE, send_words, 0)
            all_words[mine] = ring_words[...]

    for q in range(CHUNKS):
        ups[4 + q].wait_recv()
        ups[8 + q].start()
        downs[q].wait_recv()
        downs[8 + q].start()
    ups[12].start()
    downs[12].start()
    for q in range(CHUNKS):
        downs[4 + q].wait_recv()
    downs[13].start()
    downs[14].start()
    downs[15].start()

    def words_here(offset, carry):
        sender = (mine + offset) % PLANE
        word_copy(sender, sender).wait_recv()
        return carry

    lax.fori_loop(1, PLANE, words_here, 0)
    lane2 = lax.broadcasted_iota(jnp.int32, (2, WIN), 1)
    for owner in range(Y):
        for part in range(2):
            base = 4 * (2 * owner + part)
            for g in range(8):
                a = all_words[4 * g + part, owner]
                b = all_words[4 * g + 2 + part, owner]
                flat_words[base : base + 2, WIN * g : WIN * (g + 1)] = jnp.where(
                    lane2 < 64, a, pltpu.roll(b, 64, 1))
                flat_words[base + 2 : base + 4, WIN * g : WIN * (g + 1)] = jnp.where(
                    lane2 < 64, pltpu.roll(a, 64, 1), b)
    shifts = lax.broadcasted_iota(jnp.int32, (32, 1024), 0)

    def unpack(n, carry):
        row = jnp.broadcast_to(flat_words[pl.ds(n, 1), :], (32, 1024))
        bit = (lax.shift_right_logical(row, shifts) & 1).astype(jnp.float32)
        bits[pl.ds(pl.multiple_of(32 * n, 32), 32), :] = bit.astype(jnp.bfloat16)
        return carry

    lax.fori_loop(0, 32, unpack, 0)
    here = bits[:, pl.ds(pl.multiple_of(y * ROWS, ROWS), ROWS)]
    counts = lax.dot_general(here, bits[...], TN, preferred_element_type=jnp.float32)
    inverse[...] = 1.0 / jnp.maximum(counts, 1.0)
    kept_at = pl.multiple_of(zl * SIDE, SIDE)
    away_at = pl.multiple_of((1 - zl) * SIDE, SIDE)

    def encode(values):
        top = jnp.maximum(jnp.max(jnp.abs(values), axis=0, keepdims=True), 1e-30)
        codes = jnp.round(values * (32767.0 / top)).astype(jnp.int32).astype(jnp.int16)
        return codes, top / 32767.0

    def decode(codes, scale):
        return codes.astype(jnp.int32).astype(jnp.float32) * scale

    def multiply(shift, half=None, late=None):
        count = 4 if half is None else 2
        width = STA * count
        group = 4 * ((y + shift) % Y) + (0 if half is None else 2 * half)

        def product(first, last):
            right = jnp.concatenate(
                [gathered[(y + k) % Y, part, pl.ds(group, count)].reshape(width, 2 * WIN)
                 for k in OWNERS[first:last] for part in range(2)], axis=1)
            return lax.dot_general(
                turned[:, 512 * first : 512 * last], right, NT, preferred_element_type=jnp.float32)

        if late is None:
            both = product(0, 4)
        else:
            both = product(0, 3)
            late.wait_recv()
            both = both + product(3, 4)
        at = slice(SIDE, ROWS) if half == 1 else slice(0, width)
        slot = shift if half is None else shift + half
        col = pl.multiple_of(group * STA, SIDE)
        scale = inverse[:, pl.ds(col, width)]
        block[shift, :, :, at] = both.reshape(2, ROWS, width) * scale
        for plane in range(2):
            side_out[shift, plane, :, at], side_scale_out[slot, plane : plane + 1, 0:width] = encode(
                block[shift, plane, pl.ds(away_at, SIDE), at])
        copies = [
            pltpu.make_async_remote_copy(
                source, target, side_send.at[kind, slot], side_recv.at[kind, slot],
                device_id=(2 * y + 1 - zl, freq), device_id_type=MESH)
            for kind, (source, target) in enumerate((
                (side_scale_out.at[slot], side_scale_in.at[slot]),
                (side_out.at[shift, :, :, at], side_in.at[shift, :, :, at])))
        ]
        for copy in copies:
            copy.start()
        out_ref[zl, :, :, pl.ds(col, width)] = block[shift, :, pl.ds(kept_at, SIDE), at]
        return copies

    for q in range(CHUNKS):
        ups[q].wait_recv()
        ups[8 + q].wait_recv()
        downs[8 + q].wait_recv()
    for n, k in enumerate(OWNERS):
        for part in range(2):
            left = gathered[(y + k) % Y, part, pl.ds(4 * y, 4)].reshape(ROWS, 2 * WIN)
            at = (2 * n + part) * 256
            turned[0:ROWS, at : at + 256] = left
            turned[ROWS : 2 * ROWS, at : at + 256] = jnp.concatenate(
                [left[:, WIN:], -left[:, :WIN]], axis=1)
    sides = [multiply(1)]
    for plane, sign in ((0, 1.0), (1, -1.0)):
        flipped = sign * jnp.transpose(block[1, plane])
        for h in range(2):
            mirror_out[h, plane], mirror_scale_out[h, plane : plane + 1] = encode(
                flipped[SIDE * h : SIDE * (h + 1)])
    mirrors = [
        pltpu.make_async_remote_copy(
            source.at[part], target.at[zl],
            mirror_send.at[kind, n], mirror_recv.at[kind, n], device_id=device, device_id_type=MESH)
        for n, (part, device) in enumerate(((zl, ring_device(1)), (1 - zl, cross_device(1))))
        for kind, (source, target) in enumerate(
            ((mirror_scale_out, mirror_scale_in), (mirror_out, mirror_in)))
    ]
    for copy in mirrors:
        copy.start()
    ups[13].start()
    sides.append(multiply(0))
    ups[12].wait_recv()
    downs[12].wait_recv()
    sides.append(multiply(2, 0, downs[13]))
    ups[13].wait_recv()
    downs[14].wait_recv()
    sides.append(multiply(2, 1, downs[15]))

    def column(shift, half=None):
        if half is None:
            return pl.ds(pl.multiple_of(((y + shift) % Y) * ROWS, ROWS), ROWS)
        return pl.ds(pl.multiple_of(((y + shift) % Y) * ROWS + SIDE * half, SIDE), SIDE)

    stores = []

    def store(which, columns):
        copy = pltpu.make_async_copy(
            out_ref.at[which, :, :, columns], out_hbm.at[which, :, :, columns], out_sem.at[len(stores)])
        copy.start()
        stores.append(copy)

    for shift in range(3):
        store(zl, column(shift))
    for shift in (1, 0):
        for copy in sides[1 - shift]:
            copy.wait()
        for plane in range(2):
            out_ref[1 - zl, plane, :, column(shift)] = decode(
                side_in[shift, plane], side_scale_in[shift, plane : plane + 1])
        store(1 - zl, column(shift))
    for copy in mirrors:
        copy.wait()
    for n in range(2):
        for plane in range(2):
            out_ref[n, plane, :, column(3)] = decode(
                mirror_in[n, plane], mirror_scale_in[n, plane : plane + 1])
        store(n, column(3))

    def sent(offset, carry):
        other = (mine + offset) % PLANE
        for q in range(CHUNKS):
            plane_copy(q, mine, other).wait_send()
        word_copy(mine, other).wait_send()
        return carry

    lax.fori_loop(1, PLANE, sent, 0)
    for copy in ups + downs:
        copy.wait_send()
    for half in range(2):
        for copy in sides[2 + half]:
            copy.wait()
        for plane in range(2):
            out_ref[1 - zl, plane, :, column(2, half)] = decode(
                side_in[2, plane, :, SIDE * half : SIDE * (half + 1)],
                side_scale_in[2 + half, plane : plane + 1, 0:SIDE])
        store(1 - zl, column(2, half))
    for copy in stores:
        copy.wait()


def stack_up(records, table, flags, mask):
    dma = pltpu.SemaphoreType.DMA
    anywhere = pl.BlockSpec(memory_space=pl.ANY)
    return pl.pallas_call(
        kernel,
        out_shape=jax.ShapeDtypeStruct((2, 2, SIDE, 1024), jnp.float32),
        in_specs=[anywhere] * 4,
        out_specs=anywhere,
        scratch_shapes=[
            pltpu.VMEM((STA, WIN, LEN), jnp.bfloat16),
            pltpu.VMEM((2 * SLOTS, LEN), jnp.bfloat16),
            pltpu.VMEM((4, STA), jnp.int32),
            pltpu.VMEM((1, STA), jnp.int32),
            pltpu.VMEM((2, 2, SIDE, 1024), jnp.float32),
            pltpu.VMEM((8, WIN), jnp.int32),
            pltpu.VMEM((WIN, WIN), jnp.int32),
            pltpu.VMEM((2, WIN), jnp.int32),
            pltpu.VMEM((STA, WIN), jnp.float32),
            pltpu.VMEM((PART * SLOTS, WIN), jnp.float32),
            pltpu.VMEM((PART * SLOTS, WIN), jnp.float32),
            pltpu.VMEM((PLANE, STA, 2 * WIN), jnp.bfloat16),
            pltpu.VMEM((Y, 2, 16, STA, 2 * WIN), jnp.bfloat16),
            pltpu.VMEM((2 * ROWS, 2048), jnp.bfloat16),
            pltpu.VMEM((3, 2, ROWS, ROWS), jnp.float32),
            pltpu.VMEM((Y, 2, WIN), jnp.int32),
            pltpu.VMEM((PLANE, Y, 2, WIN), jnp.int32),
            pltpu.VMEM((PLANE, 1024), jnp.int32),
            pltpu.VMEM((1024, 1024), jnp.bfloat16),
            pltpu.VMEM((ROWS, 1024), jnp.float32),
            pltpu.VMEM((3, 2, SIDE, ROWS), jnp.int16),
            pltpu.VMEM((3, 2, SIDE, ROWS), jnp.int16),
            pltpu.VMEM((2, 2, SIDE, ROWS), jnp.int16),
            pltpu.VMEM((2, 2, SIDE, ROWS), jnp.int16),
            pltpu.VMEM((4, 2, ROWS), jnp.float32),
            pltpu.VMEM((4, 2, ROWS), jnp.float32),
            pltpu.VMEM((2, 2, ROWS), jnp.float32),
            pltpu.VMEM((2, 2, ROWS), jnp.float32),
            dma((CHUNKS,)), dma((3,)), dma((9,)), dma((CHUNKS, PLANE)), dma((CHUNKS, PLANE)),
            dma((Y,)), dma((Y,)), dma((PLANE,)), dma((PLANE,)),
            dma((len(UP),)), dma((len(UP),)), dma((len(DOWN),)), dma((len(DOWN),)),
            dma((2, 4)), dma((2, 4)), dma((2, 2)), dma((2, 2)),
        ],
        compiler_params=pltpu.CompilerParams(
            collective_id=0, has_side_effects=True, vmem_limit_bytes=60 << 20),
    )(records, table, flags, mask)


def local(records, gap_flags, station_mask):
    return stack_up(records, transform_table(), gap_flags.T, station_mask[None])


def solution(mesh):
    placed = (P("freq", "tm", None), P("freq", "tm"), P("freq"))
    return jax.shard_map(
        local, mesh=mesh, in_specs=placed, out_specs=P("freq", None, "tm", None), check_vma=False
    )
```

```python
import math

import jax
import jax.numpy as jnp
from jax import lax
from jax.experimental import pallas as pl
from jax.experimental.pallas import tpu as pltpu
from jax.sharding import PartitionSpec as P

FLOOR = 0.25
MESH = pl.DeviceIdType.MESH
Y = 4
PLANE = 32
STA = 64
CHUNKS = 4
PART = STA // CHUNKS
WIN = 128
LEN = 512
ROWS = 256
SIDE = 128
STEP = 8
SLOTS = 40
NEAR = (0, 1, 3, 2)
OWNERS = (0, 1, 3, 2)
NT = (((1,), (1,)), ((), ()))
TN = (((0,), (0,)), ((), ()))
QUARTERS = tuple(("q", q) for q in range(CHUNKS))
FIRST, SECOND = ("h", 0), ("h", 1)
UP = (
    [("own", 1, q) for q in QUARTERS]
    + [("own", 2, q) for q in QUARTERS]
    + [("fwd", 2, q) for q in QUARTERS]
    + [("own", 3, FIRST), ("own", 3, SECOND)]
)
DOWN = (
    [("own", 3, q) for q in QUARTERS]
    + [("own", 0, q) for q in QUARTERS]
    + [("fwd", 3, q) for q in QUARTERS]
    + [("own", 1, FIRST), ("fwd", 0, FIRST), ("own", 1, SECOND), ("fwd", 0, SECOND)]
)


def turn(phase):
    quarter = (phase + 64) // 128
    a = (phase - 128 * quarter).astype(jnp.float32) * (2.0 * math.pi / LEN)
    b = a * a
    c = 1.0 + b * (-0.5 + b * (1.0 / 24 + b * (-1.0 / 720 + b * (1.0 / 40320))))
    s = a * (1.0 + b * (-1.0 / 6 + b * (1.0 / 120 + b * (-1.0 / 5040 + b * (1.0 / 362880)))))
    odd = quarter % 2 == 1
    cosine = jnp.where(odd, s, c)
    sine = jnp.where(odd, c, s)
    cosine = jnp.where((quarter == 1) | (quarter == 2), -cosine, cosine)
    sine = jnp.where((quarter == 2) | (quarter == 3), -sine, sine)
    return cosine, sine


def transform_table():
    row = lax.broadcasted_iota(jnp.int32, (SLOTS, LEN), 0)
    t = lax.broadcasted_iota(jnp.int32, (SLOTS, LEN), 1)
    b = 5 * (row % 8) + row // 8
    taper = jnp.where(b < 36, (0.5 - 0.5 * turn(t)[0]) * (1.0 / math.sqrt(LEN)), 0.0)
    cosine, sine = turn((b * t) % LEN)
    return jnp.concatenate([cosine * taper, -sine * taper], axis=0).astype(jnp.bfloat16)


def kernel(
    rec_hbm, flag_ref, out_ref,
    rec, table_ref, kept, square, word_ref, usable, stage_re, stage_im, spec, gathered, turned, block,
    ring_words, all_words, flat_words, bits, inverse, side_out, side_in, mirror_out, mirror_in,
    side_scale_out, side_scale_in, mirror_scale_out, mirror_scale_in,
    rec_sem, plane_send, plane_recv, wring_send, wring_recv, wplane_send, wplane_recv,
    up_send, up_recv, down_send, down_recv, side_send, side_recv, mirror_send, mirror_recv,
):
    tm = lax.axis_index("tm")
    freq = lax.axis_index("freq")
    y, zl = tm // 2, tm % 2
    mine = 2 * freq + zl
    x, spot = mine // 8, mine % 8

    def plane_device(other):
        return (2 * y + other % 2, other // 2)

    def ring_device(offset):
        return (2 * ((y + offset) % Y) + zl, freq)

    def cross_device(offset):
        return (2 * ((y + offset) % Y) + 1 - zl, freq)

    loads = [
        pltpu.make_async_copy(
            rec_hbm.at[pl.ds(PART * q, PART)], rec.at[pl.ds(PART * q, PART)], rec_sem.at[q])
        for q in range(CHUNKS)
    ]
    loads[0].start()

    barrier = pltpu.get_barrier_semaphore()

    def greet(offset, carry):
        pl.semaphore_signal(
            barrier, inc=1, device_id=plane_device((mine + offset) % PLANE), device_id_type=MESH)
        return carry

    lax.fori_loop(1, PLANE, greet, 0)
    for offset in range(1, Y):
        pl.semaphore_signal(barrier, inc=1, device_id=ring_device(offset), device_id_type=MESH)
    for offset in (1, Y - 1):
        pl.semaphore_signal(barrier, inc=1, device_id=cross_device(offset), device_id_type=MESH)

    table_ref[...] = transform_table()
    kept[...] = jnp.zeros_like(kept)
    kept[0:4, 0:STA] = flag_ref[...]
    square[...] = jnp.zeros_like(square)
    square[0:8, :] = kept[...]
    words = jnp.transpose(square[...])[0:STA]
    lane = lax.broadcasted_iota(jnp.int32, (STA, WIN), 1)
    spread = jnp.broadcast_to(words[:, 0:1], (STA, WIN))
    for j in range(1, 4):
        spread = jnp.where(lane >= 32 * j, jnp.broadcast_to(words[:, j : j + 1], (STA, WIN)), spread)
    usable[...] = (lax.shift_right_logical(spread, lane % 32) & 1).astype(jnp.float32)
    low = lax.broadcasted_iota(jnp.int32, (1, WIN), 1) < STA
    rows = kept[...]
    rolled = pltpu.roll(rows, STA, 1)
    word_ref[0:1] = jnp.where(low, rows[0:1], rolled[1:2])
    word_ref[1:2] = jnp.where(low, rows[2:3], rolled[3:4])

    def transform(q):
        def pair(n, carry):
            first = PART * q + STEP * n
            both = rec[pl.ds(first, STEP)].reshape(STEP * WIN, LEN)
            spectrum = lax.dot_general(table_ref[...], both, NT, preferred_element_type=jnp.float32)
            for s in range(STEP):
                re = [spectrum[8 * v : 8 * v + 8, WIN * s : WIN * (s + 1)] for v in range(5)]
                im = [spectrum[SLOTS + 8 * v : SLOTS + 8 * v + 8, WIN * s : WIN * (s + 1)] for v in range(5)]
                m = [jnp.sqrt(a * a + b * b) for a, b in zip(re, im)]

                def above(x):
                    return pltpu.roll(x, 7, 0)

                def below(x):
                    return pltpu.roll(x, 1, 0)

                low, high = m[0] + m[1], m[3] + m[4]
                sums = [
                    low + m[2] + below(high),
                    low + m[2] + m[3] + below(m[4]),
                    low + m[2] + high,
                    m[1] + m[2] + high + above(m[0]),
                    m[2] + high + above(low),
                ]
                keep = jnp.broadcast_to(usable[pl.ds(first + s, 1), :], (8, WIN))
                for v in range(5):
                    factor = keep / jnp.maximum(sums[v] * 0.2, FLOOR)
                    at = pl.multiple_of((STEP * n + s) * SLOTS + 8 * v, 8)
                    stage_re[pl.ds(at, 8), :] = re[v] * factor
                    stage_im[pl.ds(at, 8), :] = im[v] * factor
            return carry

        lax.fori_loop(0, PART // STEP, pair, 0)
        for p in range(PLANE):
            i, v = (p + 2) // 5, (p + 2) % 5
            for half, stage in ((0, stage_re), (1, stage_im)):
                rows = stage[pl.ds(8 * v + i, PART, stride=SLOTS), :]
                spec[p, PART * q : PART * (q + 1), WIN * half : WIN * (half + 1)] = rows.astype(jnp.bfloat16)

    def plane_copy(q, sender, receiver):
        at = pl.ds(PART * q, PART)
        return pltpu.make_async_remote_copy(
            spec.at[receiver, at, :], gathered.at[y, sender % 2, sender // 2, at, :],
            plane_send.at[q, receiver], plane_recv.at[q, sender],
            device_id=plane_device(receiver), device_id_type=MESH)

    def group_peer(step, j):
        return 8 * ((x + step) % 4) + (spot + j) % 8

    def send_plane(q):
        for step in NEAR:
            def one(j, carry):
                plane_copy(q, mine, group_peer(step, j)).start()
                return carry

            lax.fori_loop(0 if step else 1, 8, one, 0)
        gathered[y, zl, freq, PART * q : PART * (q + 1), :] = spec[mine, PART * q : PART * (q + 1), :]

    def from_plane(q, step):
        def one(j, carry):
            sender = group_peer(step, j)
            plane_copy(q, sender, (sender + 1) % PLANE).wait_recv()
            return carry

        lax.fori_loop(0 if step else 1, 8, one, 0)

    for q in range(CHUNKS):
        loads[q].wait()
        if q == 0:
            for copy in loads[1:]:
                copy.start()
        transform(q)
        if q == 0:
            pl.semaphore_wait(barrier, PLANE - 1 + Y - 1 + 2)
        send_plane(q)

    ring_words[y] = word_ref[...]
    word_ring = [
        pltpu.make_async_remote_copy(
            word_ref, ring_words.at[y], wring_send.at[offset], wring_recv.at[offset],
            device_id=ring_device(offset), device_id_type=MESH)
        for offset in range(1, Y)
    ]
    for copy in word_ring:
        copy.start()

    def message(entry, slot, step, send, recv):
        kind, shift, (how, n) = entry
        owner = y if kind == "own" else (y - step + Y) % Y
        group = 4 * ((owner + shift) % Y)
        if how == "q":
            ref = gathered.at[owner, :, pl.ds(group, 4), pl.ds(PART * n, PART), :]
        else:
            ref = gathered.at[owner, :, pl.ds(group + 2 * n, 2), :, :]
        return pltpu.make_async_remote_copy(
            ref, ref, send.at[slot], recv.at[slot],
            device_id=ring_device(step % Y), device_id_type=MESH)

    ups = [message(entry, slot, 1, up_send, up_recv) for slot, entry in enumerate(UP)]
    downs = [message(entry, slot, -1, down_send, down_recv) for slot, entry in enumerate(DOWN)]

    def ring_start(q, step):
        group = (x + step) % 4
        shift = (group - y + Y) % Y
        ref = gathered.at[y, :, pl.ds(4 * group, 4), pl.ds(PART * q, PART), :]
        upward = (shift + 1) // 2 == 1

        @pl.when(upward)
        def _():
            slot = CHUNKS * (shift - 1) + q
            pltpu.make_async_remote_copy(
                ref, ref, up_send.at[slot], up_recv.at[slot],
                device_id=ring_device(1), device_id_type=MESH).start()

        @pl.when(jnp.logical_not(upward))
        def _():
            slot = CHUNKS * ((3 - shift) // 3) + q
            pltpu.make_async_remote_copy(
                ref, ref, down_send.at[slot], down_recv.at[slot],
                device_id=ring_device(Y - 1), device_id_type=MESH).start()

    for q in range(CHUNKS):
        for step in NEAR:
            from_plane(q, step)
            ring_start(q, step)
        if q == 0:
            for copy in word_ring:
                copy.wait()

            def word_copy(sender, receiver):
                return pltpu.make_async_remote_copy(
                    ring_words, all_words.at[sender],
                    wplane_send.at[receiver], wplane_recv.at[sender],
                    device_id=plane_device(receiver), device_id_type=MESH)

            def send_words(offset, carry):
                word_copy(mine, (mine + offset) % PLANE).start()
                return carry

            lax.fori_loop(1, PLANE, send_words, 0)
            all_words[mine] = ring_words[...]

    for q in range(CHUNKS):
        ups[4 + q].wait_recv()
        ups[8 + q].start()
        downs[q].wait_recv()
        downs[8 + q].start()
    ups[12].start()
    downs[12].start()
    for q in range(CHUNKS):
        downs[4 + q].wait_recv()
    downs[13].start()
    downs[14].start()
    downs[15].start()

    def words_here(offset, carry):
        sender = (mine + offset) % PLANE
        word_copy(sender, sender).wait_recv()
        return carry

    lax.fori_loop(1, PLANE, words_here, 0)
    lane2 = lax.broadcasted_iota(jnp.int32, (2, WIN), 1)
    for owner in range(Y):
        for part in range(2):
            base = 4 * (2 * owner + part)
            for g in range(8):
                a = all_words[4 * g + part, owner]
                b = all_words[4 * g + 2 + part, owner]
                flat_words[base : base + 2, WIN * g : WIN * (g + 1)] = jnp.where(
                    lane2 < 64, a, pltpu.roll(b, 64, 1))
                flat_words[base + 2 : base + 4, WIN * g : WIN * (g + 1)] = jnp.where(
                    lane2 < 64, pltpu.roll(a, 64, 1), b)
    shifts = lax.broadcasted_iota(jnp.int32, (32, 1024), 0)

    def unpack(n, carry):
        row = jnp.broadcast_to(flat_words[pl.ds(n, 1), :], (32, 1024))
        bit = (lax.shift_right_logical(row, shifts) & 1).astype(jnp.float32)
        bits[pl.ds(pl.multiple_of(32 * n, 32), 32), :] = bit.astype(jnp.bfloat16)
        return carry

    lax.fori_loop(0, 32, unpack, 0)
    here = bits[:, pl.ds(pl.multiple_of(y * ROWS, ROWS), ROWS)]
    counts = lax.dot_general(here, bits[...], TN, preferred_element_type=jnp.float32)
    inverse[...] = 1.0 / jnp.maximum(counts, 1.0)
    kept_at = pl.multiple_of(zl * SIDE, SIDE)
    away_at = pl.multiple_of((1 - zl) * SIDE, SIDE)

    def encode(values):
        top = jnp.maximum(jnp.max(jnp.abs(values), axis=0, keepdims=True), 1e-30)
        codes = jnp.round(values * (32767.0 / top)).astype(jnp.int32).astype(jnp.int16)
        return codes, top / 32767.0

    def decode(codes, scale):
        return codes.astype(jnp.int32).astype(jnp.float32) * scale

    def swap(shift, slot, at, width):
        for plane in range(2):
            side_out[shift, plane, :, at], side_scale_out[slot, plane : plane + 1, 0:width] = encode(
                block[shift, plane, pl.ds(away_at, SIDE), at])
        copies = [
            pltpu.make_async_remote_copy(
                source, target, side_send.at[kind, slot], side_recv.at[kind, slot],
                device_id=(2 * y + 1 - zl, freq), device_id_type=MESH)
            for kind, (source, target) in enumerate((
                (side_scale_out.at[slot], side_scale_in.at[slot]),
                (side_out.at[shift, :, :, at], side_in.at[shift, :, :, at])))
        ]
        for copy in copies:
            copy.start()
        return copies

    def right_side(group, count, first, last):
        return jnp.concatenate(
            [gathered[(y + k) % Y, part, pl.ds(group, count)].reshape(STA * count, 2 * WIN)
             for k in OWNERS[first:last] for part in range(2)], axis=1)

    def multiply(shift):
        both = lax.dot_general(
            turned[...], right_side(4 * ((y + shift) % Y), 4, 0, 4), NT,
            preferred_element_type=jnp.float32)
        col = pl.multiple_of(((y + shift) % Y) * ROWS, ROWS)
        block[shift] = both.reshape(2, ROWS, ROWS) * inverse[:, pl.ds(col, ROWS)]
        copies = swap(shift, shift, slice(0, ROWS), ROWS)
        out_ref[zl, :, :, pl.ds(col, ROWS)] = block[shift, :, pl.ds(kept_at, SIDE), :]
        return copies

    def multiply_late(half, late):
        group = 4 * ((y + 2) % Y) + 2 * half
        at = slice(SIDE * half, SIDE * (half + 1))
        col = pl.multiple_of(group * STA, SIDE)
        early = lax.dot_general(
            turned[:, 0:1536], right_side(group, 2, 0, 3), NT, preferred_element_type=jnp.float32)
        block[2, :, :, at] = early.reshape(2, ROWS, SIDE)
        late.wait_recv()
        right = right_side(group, 2, 3, 4)

        def finish(rows):
            left = jnp.concatenate(
                [turned[pl.ds(rows + start, SIDE), 1536:2048] for start in (0, ROWS)], axis=0)
            both = lax.dot_general(left, right, NT, preferred_element_type=jnp.float32)
            block[2, :, pl.ds(rows, SIDE), at] = (
                block[2, :, pl.ds(rows, SIDE), at] + both.reshape(2, SIDE, SIDE)
            ) * inverse[pl.ds(rows, SIDE), pl.ds(col, SIDE)]

        finish(away_at)
        copies = swap(2, 2 + half, at, SIDE)
        finish(kept_at)
        out_ref[zl, :, :, pl.ds(col, SIDE)] = block[2, :, pl.ds(kept_at, SIDE), at]
        return copies

    for q in range(CHUNKS):
        ups[q].wait_recv()
        ups[8 + q].wait_recv()
        downs[8 + q].wait_recv()
    for n, k in enumerate(OWNERS):
        for part in range(2):
            left = gathered[(y + k) % Y, part, pl.ds(4 * y, 4)].reshape(ROWS, 2 * WIN)
            at = (2 * n + part) * 256
            turned[0:ROWS, at : at + 256] = left
            turned[ROWS : 2 * ROWS, at : at + 256] = jnp.concatenate(
                [left[:, WIN:], -left[:, :WIN]], axis=1)
    sides = [multiply(1)]
    for plane, sign in ((0, 1.0), (1, -1.0)):
        flipped = sign * jnp.transpose(block[1, plane])
        for h in range(2):
            mirror_out[h, plane], mirror_scale_out[h, plane : plane + 1] = encode(
                flipped[SIDE * h : SIDE * (h + 1)])
    mirrors = [
        pltpu.make_async_remote_copy(
            source.at[part], target.at[zl],
            mirror_send.at[kind, n], mirror_recv.at[kind, n], device_id=device, device_id_type=MESH)
        for n, (part, device) in enumerate(((zl, ring_device(1)), (1 - zl, cross_device(1))))
        for kind, (source, target) in enumerate(
            ((mirror_scale_out, mirror_scale_in), (mirror_out, mirror_in)))
    ]
    for copy in mirrors:
        copy.start()
    ups[13].start()
    sides.append(multiply(0))
    ups[12].wait_recv()
    downs[12].wait_recv()
    sides.append(multiply_late(0, downs[13]))
    ups[13].wait_recv()
    downs[14].wait_recv()
    sides.append(multiply_late(1, downs[15]))

    def column(shift, half=None):
        if half is None:
            return pl.ds(pl.multiple_of(((y + shift) % Y) * ROWS, ROWS), ROWS)
        return pl.ds(pl.multiple_of(((y + shift) % Y) * ROWS + SIDE * half, SIDE), SIDE)

    for shift in (1, 0):
        for copy in sides[1 - shift]:
            copy.wait()
        for plane in range(2):
            out_ref[1 - zl, plane, :, column(shift)] = decode(
                side_in[shift, plane], side_scale_in[shift, plane : plane + 1])
    for copy in mirrors:
        copy.wait()
    for n in range(2):
        for plane in range(2):
            out_ref[n, plane, :, column(3)] = decode(
                mirror_in[n, plane], mirror_scale_in[n, plane : plane + 1])

    def sent(offset, carry):
        other = (mine + offset) % PLANE
        for q in range(CHUNKS):
            plane_copy(q, mine, other).wait_send()
        word_copy(mine, other).wait_send()
        return carry

    lax.fori_loop(1, PLANE, sent, 0)
    for copy in ups + downs:
        copy.wait_send()
    for half in range(2):
        for copy in sides[2 + half]:
            copy.wait()
        for plane in range(2):
            out_ref[1 - zl, plane, :, column(2, half)] = decode(
                side_in[2, plane, :, SIDE * half : SIDE * (half + 1)],
                side_scale_in[2 + half, plane : plane + 1, 0:SIDE])


def stack_up(records, flags):
    dma = pltpu.SemaphoreType.DMA
    vmem = pl.BlockSpec(memory_space=pltpu.VMEM)
    return pl.pallas_call(
        kernel,
        out_shape=jax.ShapeDtypeStruct((2, 2, SIDE, 1024), jnp.float32),
        in_specs=[pl.BlockSpec(memory_space=pl.ANY), vmem],
        out_specs=vmem,
        scratch_shapes=[
            pltpu.VMEM((STA, WIN, LEN), jnp.bfloat16),
            pltpu.VMEM((2 * SLOTS, LEN), jnp.bfloat16),
            pltpu.VMEM((8, WIN), jnp.int32),
            pltpu.VMEM((WIN, WIN), jnp.int32),
            pltpu.VMEM((2, WIN), jnp.int32),
            pltpu.VMEM((STA, WIN), jnp.float32),
            pltpu.VMEM((PART * SLOTS, WIN), jnp.float32),
            pltpu.VMEM((PART * SLOTS, WIN), jnp.float32),
            pltpu.VMEM((PLANE, STA, 2 * WIN), jnp.bfloat16),
            pltpu.VMEM((Y, 2, 16, STA, 2 * WIN), jnp.bfloat16),
            pltpu.VMEM((2 * ROWS, 2048), jnp.bfloat16),
            pltpu.VMEM((3, 2, ROWS, ROWS), jnp.float32),
            pltpu.VMEM((Y, 2, WIN), jnp.int32),
            pltpu.VMEM((PLANE, Y, 2, WIN), jnp.int32),
            pltpu.VMEM((PLANE, 1024), jnp.int32),
            pltpu.VMEM((1024, 1024), jnp.bfloat16),
            pltpu.VMEM((ROWS, 1024), jnp.float32),
            pltpu.VMEM((3, 2, SIDE, ROWS), jnp.int16),
            pltpu.VMEM((3, 2, SIDE, ROWS), jnp.int16),
            pltpu.VMEM((2, 2, SIDE, ROWS), jnp.int16),
            pltpu.VMEM((2, 2, SIDE, ROWS), jnp.int16),
            pltpu.VMEM((4, 2, ROWS), jnp.float32),
            pltpu.VMEM((4, 2, ROWS), jnp.float32),
            pltpu.VMEM((2, 2, ROWS), jnp.float32),
            pltpu.VMEM((2, 2, ROWS), jnp.float32),
            dma((CHUNKS,)), dma((CHUNKS, PLANE)), dma((CHUNKS, PLANE)),
            dma((Y,)), dma((Y,)), dma((PLANE,)), dma((PLANE,)),
            dma((len(UP),)), dma((len(UP),)), dma((len(DOWN),)), dma((len(DOWN),)),
            dma((2, 4)), dma((2, 4)), dma((2, 2)), dma((2, 2)),
        ],
        compiler_params=pltpu.CompilerParams(
            collective_id=0, has_side_effects=True, vmem_limit_bytes=48 << 20),
    )(records, flags)


def local(records, gap_flags, station_mask):
    return stack_up(records, gap_flags.T * station_mask[None])


def solution(mesh):
    placed = (P("freq", "tm", None), P("freq", "tm"), P("freq"))
    return jax.shard_map(
        local, mesh=mesh, in_specs=placed, out_specs=P("freq", None, "tm", None), check_vma=False
    )
```

```python
import math

import jax
import jax.numpy as jnp
from jax import lax
from jax.experimental import pallas as pl
from jax.experimental.pallas import tpu as pltpu
from jax.sharding import PartitionSpec as P

FLOOR = 0.25
MESH = pl.DeviceIdType.MESH
Y = 4
PLANE = 32
STA = 64
CHUNKS = 4
PART = STA // CHUNKS
WIN = 128
LEN = 512
ROWS = 256
SIDE = 128
STEP = 8
SLOTS = 40
NEAR = (0, 1, 3, 2)
OWNERS = (0, 1, 3, 2)
NT = (((1,), (1,)), ((), ()))
TN = (((0,), (0,)), ((), ()))
QUARTERS = tuple(("q", q) for q in range(CHUNKS))
FIRST, SECOND = ("h", 0), ("h", 1)
UP = (
    [("own", 1, q) for q in QUARTERS]
    + [("own", 2, q) for q in QUARTERS]
    + [("fwd", 2, q) for q in QUARTERS]
    + [("own", 3, FIRST), ("own", 3, SECOND)]
)
DOWN = (
    [("own", 3, q) for q in QUARTERS]
    + [("own", 0, q) for q in QUARTERS]
    + [("fwd", 3, q) for q in QUARTERS]
    + [("own", 1, FIRST), ("fwd", 0, FIRST), ("own", 1, SECOND), ("fwd", 0, SECOND)]
)


def turn(phase):
    quarter = (phase + 64) // 128
    a = (phase - 128 * quarter).astype(jnp.float32) * (2.0 * math.pi / LEN)
    b = a * a
    c = 1.0 + b * (-0.5 + b * (1.0 / 24 + b * (-1.0 / 720 + b * (1.0 / 40320))))
    s = a * (1.0 + b * (-1.0 / 6 + b * (1.0 / 120 + b * (-1.0 / 5040 + b * (1.0 / 362880)))))
    odd = quarter % 2 == 1
    cosine = jnp.where(odd, s, c)
    sine = jnp.where(odd, c, s)
    cosine = jnp.where((quarter == 1) | (quarter == 2), -cosine, cosine)
    sine = jnp.where((quarter == 2) | (quarter == 3), -sine, sine)
    return cosine, sine


def transform_table():
    row = lax.broadcasted_iota(jnp.int32, (SLOTS, LEN), 0)
    t = lax.broadcasted_iota(jnp.int32, (SLOTS, LEN), 1)
    b = 5 * (row % 8) + row // 8
    taper = jnp.where(b < 36, (0.5 - 0.5 * turn(t)[0]) * (1.0 / math.sqrt(LEN)), 0.0)
    cosine, sine = turn((b * t) % LEN)
    return jnp.concatenate([cosine * taper, -sine * taper], axis=0).astype(jnp.bfloat16)


def kernel(
    rec_hbm, flag_ref, out_ref,
    rec, table_ref, kept, square, word_ref, usable, stage_re, stage_im, spec, gathered, turned, block,
    ring_words, all_words, flat_words, bits, inverse, side_out, side_in, mirror_out, mirror_in,
    side_scale_out, side_scale_in, mirror_scale_out, mirror_scale_in,
    rec_sem, plane_send, plane_recv, wring_send, wring_recv, wplane_send, wplane_recv,
    up_send, up_recv, down_send, down_recv, side_send, side_recv, mirror_send, mirror_recv,
):
    tm = lax.axis_index("tm")
    freq = lax.axis_index("freq")
    y, zl = tm // 2, tm % 2
    mine = 2 * freq + zl
    x, spot = mine // 8, mine % 8

    def plane_device(other):
        return (2 * y + other % 2, other // 2)

    def ring_device(offset):
        return (2 * ((y + offset) % Y) + zl, freq)

    def cross_device(offset):
        return (2 * ((y + offset) % Y) + 1 - zl, freq)

    loads = [
        pltpu.make_async_copy(
            rec_hbm.at[pl.ds(PART * q, PART)], rec.at[pl.ds(PART * q, PART)], rec_sem.at[q])
        for q in range(CHUNKS)
    ]
    loads[0].start()

    barrier = pltpu.get_barrier_semaphore()

    def greet(offset, carry):
        pl.semaphore_signal(
            barrier, inc=1, device_id=plane_device((mine + offset) % PLANE), device_id_type=MESH)
        return carry

    for offset in range(1, PLANE):
        greet(offset, 0)
    for offset in range(1, Y):
        pl.semaphore_signal(barrier, inc=1, device_id=ring_device(offset), device_id_type=MESH)
    for offset in (1, Y - 1):
        pl.semaphore_signal(barrier, inc=1, device_id=cross_device(offset), device_id_type=MESH)

    table_ref[...] = transform_table()
    kept[...] = jnp.zeros_like(kept)
    kept[0:4, 0:STA] = flag_ref[...]
    square[...] = jnp.zeros_like(square)
    square[0:8, :] = kept[...]
    words = jnp.transpose(square[...])[0:STA]
    lane = lax.broadcasted_iota(jnp.int32, (STA, WIN), 1)
    spread = jnp.broadcast_to(words[:, 0:1], (STA, WIN))
    for j in range(1, 4):
        spread = jnp.where(lane >= 32 * j, jnp.broadcast_to(words[:, j : j + 1], (STA, WIN)), spread)
    usable[...] = (lax.shift_right_logical(spread, lane % 32) & 1).astype(jnp.float32)
    low = lax.broadcasted_iota(jnp.int32, (1, WIN), 1) < STA
    rows = kept[...]
    rolled = pltpu.roll(rows, STA, 1)
    word_ref[0:1] = jnp.where(low, rows[0:1], rolled[1:2])
    word_ref[1:2] = jnp.where(low, rows[2:3], rolled[3:4])

    def transform(q):
        def pair(n, carry):
            first = PART * q + STEP * n
            both = rec[pl.ds(first, STEP)].reshape(STEP * WIN, LEN)
            spectrum = lax.dot_general(table_ref[...], both, NT, preferred_element_type=jnp.float32)
            for s in range(STEP):
                re = [spectrum[8 * v : 8 * v + 8, WIN * s : WIN * (s + 1)] for v in range(5)]
                im = [spectrum[SLOTS + 8 * v : SLOTS + 8 * v + 8, WIN * s : WIN * (s + 1)] for v in range(5)]
                m = [jnp.sqrt(a * a + b * b) for a, b in zip(re, im)]

                def above(x):
                    return pltpu.roll(x, 7, 0)

                def below(x):
                    return pltpu.roll(x, 1, 0)

                low, high = m[0] + m[1], m[3] + m[4]
                sums = [
                    low + m[2] + below(high),
                    low + m[2] + m[3] + below(m[4]),
                    low + m[2] + high,
                    m[1] + m[2] + high + above(m[0]),
                    m[2] + high + above(low),
                ]
                keep = jnp.broadcast_to(usable[pl.ds(first + s, 1), :], (8, WIN))
                for v in range(5):
                    factor = keep / jnp.maximum(sums[v] * 0.2, FLOOR)
                    at = pl.multiple_of((STEP * n + s) * SLOTS + 8 * v, 8)
                    stage_re[pl.ds(at, 8), :] = re[v] * factor
                    stage_im[pl.ds(at, 8), :] = im[v] * factor
            return carry

        lax.fori_loop(0, PART // STEP, pair, 0)
        for p in range(PLANE):
            i, v = (p + 2) // 5, (p + 2) % 5
            for half, stage in ((0, stage_re), (1, stage_im)):
                rows = stage[pl.ds(8 * v + i, PART, stride=SLOTS), :]
                spec[p, PART * q : PART * (q + 1), WIN * half : WIN * (half + 1)] = rows.astype(jnp.bfloat16)

    def plane_copy(q, sender, receiver):
        at = pl.ds(PART * q, PART)
        return pltpu.make_async_remote_copy(
            spec.at[receiver, at, :], gathered.at[y, sender % 2, sender // 2, at, :],
            plane_send.at[q, receiver], plane_recv.at[q, sender],
            device_id=plane_device(receiver), device_id_type=MESH)

    def group_peer(step, j):
        return 8 * ((x + step) % 4) + (spot + j) % 8

    def send_plane(q):
        for step in NEAR:
            for j in range(0 if step else 1, 8):
                plane_copy(q, mine, group_peer(step, j)).start()
        gathered[y, zl, freq, PART * q : PART * (q + 1), :] = spec[mine, PART * q : PART * (q + 1), :]

    def from_plane(q, step):
        for j in range(0 if step else 1, 8):
            sender = group_peer(step, j)
            plane_copy(q, sender, (sender + 1) % PLANE).wait_recv()

    for q in range(CHUNKS):
        loads[q].wait()
        if q == 0:
            for copy in loads[1:]:
                copy.start()
        transform(q)
        if q == 0:
            pl.semaphore_wait(barrier, PLANE - 1 + Y - 1 + 2)
        send_plane(q)

    ring_words[y] = word_ref[...]
    word_ring = [
        pltpu.make_async_remote_copy(
            word_ref, ring_words.at[y], wring_send.at[offset], wring_recv.at[offset],
            device_id=ring_device(offset), device_id_type=MESH)
        for offset in range(1, Y)
    ]
    for copy in word_ring:
        copy.start()

    def message(entry, slot, step, send, recv):
        kind, shift, (how, n) = entry
        owner = y if kind == "own" else (y - step + Y) % Y
        group = 4 * ((owner + shift) % Y)
        if how == "q":
            ref = gathered.at[owner, :, pl.ds(group, 4), pl.ds(PART * n, PART), :]
        else:
            ref = gathered.at[owner, :, pl.ds(group + 2 * n, 2), :, :]
        return pltpu.make_async_remote_copy(
            ref, ref, send.at[slot], recv.at[slot],
            device_id=ring_device(step % Y), device_id_type=MESH)

    ups = [message(entry, slot, 1, up_send, up_recv) for slot, entry in enumerate(UP)]
    downs = [message(entry, slot, -1, down_send, down_recv) for slot, entry in enumerate(DOWN)]

    def ring_start(q, step):
        group = (x + step) % 4
        shift = (group - y + Y) % Y
        ref = gathered.at[y, :, pl.ds(4 * group, 4), pl.ds(PART * q, PART), :]
        upward = (shift + 1) // 2 == 1

        @pl.when(upward)
        def _():
            slot = CHUNKS * (shift - 1) + q
            pltpu.make_async_remote_copy(
                ref, ref, up_send.at[slot], up_recv.at[slot],
                device_id=ring_device(1), device_id_type=MESH).start()

        @pl.when(jnp.logical_not(upward))
        def _():
            slot = CHUNKS * ((3 - shift) // 3) + q
            pltpu.make_async_remote_copy(
                ref, ref, down_send.at[slot], down_recv.at[slot],
                device_id=ring_device(Y - 1), device_id_type=MESH).start()

    for q in range(CHUNKS):
        for step in NEAR:
            from_plane(q, step)
            ring_start(q, step)
        if q == 0:
            for copy in word_ring:
                copy.wait()

            def word_copy(sender, receiver):
                return pltpu.make_async_remote_copy(
                    ring_words, all_words.at[sender],
                    wplane_send.at[receiver], wplane_recv.at[sender],
                    device_id=plane_device(receiver), device_id_type=MESH)

            def send_words(offset, carry):
                word_copy(mine, (mine + offset) % PLANE).start()
                return carry

            lax.fori_loop(1, PLANE, send_words, 0)
            all_words[mine] = ring_words[...]

    for q in range(CHUNKS):
        ups[4 + q].wait_recv()
        ups[8 + q].start()
        downs[q].wait_recv()
        downs[8 + q].start()
    ups[12].start()
    downs[12].start()
    ups[13].start()
    for q in range(CHUNKS):
        downs[4 + q].wait_recv()
    downs[13].start()
    downs[14].start()
    downs[15].start()

    def words_here(offset, carry):
        sender = (mine + offset) % PLANE
        word_copy(sender, sender).wait_recv()
        return carry

    lax.fori_loop(1, PLANE, words_here, 0)
    lane2 = lax.broadcasted_iota(jnp.int32, (2, WIN), 1)
    for owner in range(Y):
        for part in range(2):
            base = 4 * (2 * owner + part)
            for g in range(8):
                a = all_words[4 * g + part, owner]
                b = all_words[4 * g + 2 + part, owner]
                flat_words[base : base + 2, WIN * g : WIN * (g + 1)] = jnp.where(
                    lane2 < 64, a, pltpu.roll(b, 64, 1))
                flat_words[base + 2 : base + 4, WIN * g : WIN * (g + 1)] = jnp.where(
                    lane2 < 64, pltpu.roll(a, 64, 1), b)
    shifts = lax.broadcasted_iota(jnp.int32, (32, 1024), 0)

    def unpack(n, carry):
        row = jnp.broadcast_to(flat_words[pl.ds(n, 1), :], (32, 1024))
        bit = (lax.shift_right_logical(row, shifts) & 1).astype(jnp.float32)
        bits[pl.ds(pl.multiple_of(32 * n, 32), 32), :] = bit.astype(jnp.bfloat16)
        return carry

    lax.fori_loop(0, 32, unpack, 0)
    here = bits[:, pl.ds(pl.multiple_of(y * ROWS, ROWS), ROWS)]
    counts = lax.dot_general(here, bits[...], TN, preferred_element_type=jnp.float32)
    inverse[...] = 1.0 / jnp.maximum(counts, 1.0)
    kept_at = pl.multiple_of(zl * SIDE, SIDE)
    away_at = pl.multiple_of((1 - zl) * SIDE, SIDE)

    def encode(values):
        top = jnp.maximum(jnp.max(jnp.abs(values), axis=0, keepdims=True), 1e-30)
        codes = jnp.round(values * (32767.0 / top)).astype(jnp.int32).astype(jnp.int16)
        return codes, top / 32767.0

    def decode(codes, scale):
        return codes.astype(jnp.int32).astype(jnp.float32) * scale

    def swap(shift, slot, at, width):
        for plane in range(2):
            side_out[shift, plane, :, at], side_scale_out[slot, plane : plane + 1, 0:width] = encode(
                block[shift, plane, pl.ds(away_at, SIDE), at])
        copies = [
            pltpu.make_async_remote_copy(
                source, target, side_send.at[kind, slot], side_recv.at[kind, slot],
                device_id=(2 * y + 1 - zl, freq), device_id_type=MESH)
            for kind, (source, target) in enumerate((
                (side_scale_out.at[slot], side_scale_in.at[slot]),
                (side_out.at[shift, :, :, at], side_in.at[shift, :, :, at])))
        ]
        for copy in copies:
            copy.start()
        return copies

    def right_side(group, count, first, last):
        return jnp.concatenate(
            [gathered[(y + k) % Y, part, pl.ds(group, count)].reshape(STA * count, 2 * WIN)
             for k in OWNERS[first:last] for part in range(2)], axis=1)

    def multiply(shift):
        both = lax.dot_general(
            turned[...], right_side(4 * ((y + shift) % Y), 4, 0, 4), NT,
            preferred_element_type=jnp.float32)
        col = pl.multiple_of(((y + shift) % Y) * ROWS, ROWS)
        block[shift] = both.reshape(2, ROWS, ROWS) * inverse[:, pl.ds(col, ROWS)]
        copies = swap(shift, shift, slice(0, ROWS), ROWS)
        out_ref[zl, :, :, pl.ds(col, ROWS)] = block[shift, :, pl.ds(kept_at, SIDE), :]
        return copies

    def multiply_late(half, late):
        group = 4 * ((y + 2) % Y) + 2 * half
        at = slice(SIDE * half, SIDE * (half + 1))
        col = pl.multiple_of(group * STA, SIDE)
        early = lax.dot_general(
            turned[:, 0:1536], right_side(group, 2, 0, 3), NT, preferred_element_type=jnp.float32)
        block[2, :, :, at] = early.reshape(2, ROWS, SIDE)
        late.wait_recv()
        right = right_side(group, 2, 3, 4)

        def finish(rows):
            left = jnp.concatenate(
                [turned[pl.ds(rows + start, SIDE), 1536:2048] for start in (0, ROWS)], axis=0)
            both = lax.dot_general(left, right, NT, preferred_element_type=jnp.float32)
            block[2, :, pl.ds(rows, SIDE), at] = (
                block[2, :, pl.ds(rows, SIDE), at] + both.reshape(2, SIDE, SIDE)
            ) * inverse[pl.ds(rows, SIDE), pl.ds(col, SIDE)]

        finish(away_at)
        copies = swap(2, 2 + half, at, SIDE)
        finish(kept_at)
        out_ref[zl, :, :, pl.ds(col, SIDE)] = block[2, :, pl.ds(kept_at, SIDE), at]
        return copies

    for q in range(CHUNKS):
        ups[q].wait_recv()
        ups[8 + q].wait_recv()
        downs[8 + q].wait_recv()
    for n, k in enumerate(OWNERS):
        for part in range(2):
            left = gathered[(y + k) % Y, part, pl.ds(4 * y, 4)].reshape(ROWS, 2 * WIN)
            at = (2 * n + part) * 256
            turned[0:ROWS, at : at + 256] = left
            turned[ROWS : 2 * ROWS, at : at + 256] = jnp.concatenate(
                [left[:, WIN:], -left[:, :WIN]], axis=1)
    sides = [multiply(1)]
    for plane, sign in ((0, 1.0), (1, -1.0)):
        flipped = sign * jnp.transpose(block[1, plane])
        for h in range(2):
            mirror_out[h, plane], mirror_scale_out[h, plane : plane + 1] = encode(
                flipped[SIDE * h : SIDE * (h + 1)])
    mirrors = [
        pltpu.make_async_remote_copy(
            source.at[part], target.at[zl],
            mirror_send.at[kind, n], mirror_recv.at[kind, n], device_id=device, device_id_type=MESH)
        for n, (part, device) in enumerate(((zl, ring_device(1)), (1 - zl, cross_device(1))))
        for kind, (source, target) in enumerate(
            ((mirror_scale_out, mirror_scale_in), (mirror_out, mirror_in)))
    ]
    for copy in mirrors:
        copy.start()
    sides.append(multiply(0))
    ups[12].wait_recv()
    downs[12].wait_recv()
    sides.append(multiply_late(0, downs[13]))
    ups[13].wait_recv()
    downs[14].wait_recv()
    sides.append(multiply_late(1, downs[15]))

    def column(shift, half=None):
        if half is None:
            return pl.ds(pl.multiple_of(((y + shift) % Y) * ROWS, ROWS), ROWS)
        return pl.ds(pl.multiple_of(((y + shift) % Y) * ROWS + SIDE * half, SIDE), SIDE)

    for shift in (1, 0):
        for copy in sides[1 - shift]:
            copy.wait()
        for plane in range(2):
            out_ref[1 - zl, plane, :, column(shift)] = decode(
                side_in[shift, plane], side_scale_in[shift, plane : plane + 1])
    for copy in mirrors:
        copy.wait()
    for n in range(2):
        for plane in range(2):
            out_ref[n, plane, :, column(3)] = decode(
                mirror_in[n, plane], mirror_scale_in[n, plane : plane + 1])

    def sent(offset, carry):
        other = (mine + offset) % PLANE
        for q in range(CHUNKS):
            plane_copy(q, mine, other).wait_send()
        word_copy(mine, other).wait_send()
        return carry

    lax.fori_loop(1, PLANE, sent, 0)
    for copy in ups + downs:
        copy.wait_send()
    for half in range(2):
        for copy in sides[2 + half]:
            copy.wait()
        for plane in range(2):
            out_ref[1 - zl, plane, :, column(2, half)] = decode(
                side_in[2, plane, :, SIDE * half : SIDE * (half + 1)],
                side_scale_in[2 + half, plane : plane + 1, 0:SIDE])


def stack_up(records, flags):
    dma = pltpu.SemaphoreType.DMA
    vmem = pl.BlockSpec(memory_space=pltpu.VMEM)
    return pl.pallas_call(
        kernel,
        out_shape=jax.ShapeDtypeStruct((2, 2, SIDE, 1024), jnp.float32),
        in_specs=[pl.BlockSpec(memory_space=pl.ANY), vmem],
        out_specs=vmem,
        scratch_shapes=[
            pltpu.VMEM((STA, WIN, LEN), jnp.bfloat16),
            pltpu.VMEM((2 * SLOTS, LEN), jnp.bfloat16),
            pltpu.VMEM((8, WIN), jnp.int32),
            pltpu.VMEM((WIN, WIN), jnp.int32),
            pltpu.VMEM((2, WIN), jnp.int32),
            pltpu.VMEM((STA, WIN), jnp.float32),
            pltpu.VMEM((PART * SLOTS, WIN), jnp.float32),
            pltpu.VMEM((PART * SLOTS, WIN), jnp.float32),
            pltpu.VMEM((PLANE, STA, 2 * WIN), jnp.bfloat16),
            pltpu.VMEM((Y, 2, 16, STA, 2 * WIN), jnp.bfloat16),
            pltpu.VMEM((2 * ROWS, 2048), jnp.bfloat16),
            pltpu.VMEM((3, 2, ROWS, ROWS), jnp.float32),
            pltpu.VMEM((Y, 2, WIN), jnp.int32),
            pltpu.VMEM((PLANE, Y, 2, WIN), jnp.int32),
            pltpu.VMEM((PLANE, 1024), jnp.int32),
            pltpu.VMEM((1024, 1024), jnp.bfloat16),
            pltpu.VMEM((ROWS, 1024), jnp.float32),
            pltpu.VMEM((3, 2, SIDE, ROWS), jnp.int16),
            pltpu.VMEM((3, 2, SIDE, ROWS), jnp.int16),
            pltpu.VMEM((2, 2, SIDE, ROWS), jnp.int16),
            pltpu.VMEM((2, 2, SIDE, ROWS), jnp.int16),
            pltpu.VMEM((4, 2, ROWS), jnp.float32),
            pltpu.VMEM((4, 2, ROWS), jnp.float32),
            pltpu.VMEM((2, 2, ROWS), jnp.float32),
            pltpu.VMEM((2, 2, ROWS), jnp.float32),
            dma((CHUNKS,)), dma((CHUNKS, PLANE)), dma((CHUNKS, PLANE)),
            dma((Y,)), dma((Y,)), dma((PLANE,)), dma((PLANE,)),
            dma((len(UP),)), dma((len(UP),)), dma((len(DOWN),)), dma((len(DOWN),)),
            dma((2, 4)), dma((2, 4)), dma((2, 2)), dma((2, 2)),
        ],
        compiler_params=pltpu.CompilerParams(
            collective_id=0, has_side_effects=True, vmem_limit_bytes=48 << 20),
    )(records, flags)


def local(records, gap_flags, station_mask):
    return stack_up(records, gap_flags.T * station_mask[None])


def solution(mesh):
    placed = (P("freq", "tm", None), P("freq", "tm"), P("freq"))
    return jax.shard_map(
        local, mesh=mesh, in_specs=placed, out_specs=P("freq", None, "tm", None), check_vma=False
    )
```

```python
import math

import jax
import jax.numpy as jnp
from jax import lax
from jax.experimental import pallas as pl
from jax.experimental.pallas import tpu as pltpu
from jax.sharding import PartitionSpec as P

FLOOR = 0.25
MESH = pl.DeviceIdType.MESH
Y = 4
PLANE = 32
STA = 64
CHUNKS = 4
PART = STA // CHUNKS
WIN = 128
LEN = 512
ROWS = 256
SIDE = 128
STEP = 8
SLOTS = 40
NEAR = (0, 1, 3, 2)
OWNERS = (0, 1, 3, 2)
NT = (((1,), (1,)), ((), ()))
TN = (((0,), (0,)), ((), ()))
QUARTERS = tuple(("q", q) for q in range(CHUNKS))
FIRST, SECOND = ("h", 0), ("h", 1)
UP = (
    [("own", 1, q) for q in QUARTERS]
    + [("own", 2, q) for q in QUARTERS]
    + [("fwd", 2, q) for q in QUARTERS]
    + [("own", 3, FIRST), ("own", 3, SECOND)]
)
DOWN = (
    [("own", 3, q) for q in QUARTERS]
    + [("own", 0, q) for q in QUARTERS]
    + [("fwd", 3, q) for q in QUARTERS]
    + [("own", 1, FIRST), ("fwd", 0, FIRST), ("own", 1, SECOND), ("fwd", 0, SECOND)]
)


def turn(phase):
    quarter = (phase + 64) // 128
    a = (phase - 128 * quarter).astype(jnp.float32) * (2.0 * math.pi / LEN)
    b = a * a
    c = 1.0 + b * (-0.5 + b * (1.0 / 24 + b * (-1.0 / 720 + b * (1.0 / 40320))))
    s = a * (1.0 + b * (-1.0 / 6 + b * (1.0 / 120 + b * (-1.0 / 5040 + b * (1.0 / 362880)))))
    odd = quarter % 2 == 1
    cosine = jnp.where(odd, s, c)
    sine = jnp.where(odd, c, s)
    cosine = jnp.where((quarter == 1) | (quarter == 2), -cosine, cosine)
    sine = jnp.where((quarter == 2) | (quarter == 3), -sine, sine)
    return cosine, sine


def transform_table():
    row = lax.broadcasted_iota(jnp.int32, (SLOTS, LEN), 0)
    t = lax.broadcasted_iota(jnp.int32, (SLOTS, LEN), 1)
    b = 5 * (row % 8) + row // 8
    taper = jnp.where(b < 36, (0.5 - 0.5 * turn(t)[0]) * (1.0 / math.sqrt(LEN)), 0.0)
    cosine, sine = turn((b * t) % LEN)
    return jnp.concatenate([cosine * taper, -sine * taper], axis=0).astype(jnp.bfloat16)


def kernel(
    rec_hbm, flag_ref, out_ref,
    rec, table_ref, kept, square, word_ref, usable, stage_re, stage_im, spec, gathered, turned, block,
    ring_words, all_words, flat_words, bits, inverse, side_out, side_in, mirror_out, mirror_in,
    side_scale_out, side_scale_in, mirror_scale_out, mirror_scale_in,
    rec_sem, plane_send, plane_recv, wring_send, wring_recv, wplane_send, wplane_recv,
    up_send, up_recv, down_send, down_recv, side_send, side_recv, mirror_send, mirror_recv,
):
    tm = lax.axis_index("tm")
    freq = lax.axis_index("freq")
    y, zl = tm // 2, tm % 2
    mine = 2 * freq + zl
    x, spot = mine // 8, mine % 8

    def plane_device(other):
        return (2 * y + other % 2, other // 2)

    def ring_device(offset):
        return (2 * ((y + offset) % Y) + zl, freq)

    def cross_device(offset):
        return (2 * ((y + offset) % Y) + 1 - zl, freq)

    loads = [
        pltpu.make_async_copy(
            rec_hbm.at[pl.ds(PART * q, PART)], rec.at[pl.ds(PART * q, PART)], rec_sem.at[q])
        for q in range(CHUNKS)
    ]
    loads[0].start()

    barrier = pltpu.get_barrier_semaphore()

    def greet(offset, carry):
        pl.semaphore_signal(
            barrier, inc=1, device_id=plane_device((mine + offset) % PLANE), device_id_type=MESH)
        return carry

    for offset in range(1, PLANE):
        greet(offset, 0)
    for offset in range(1, Y):
        pl.semaphore_signal(barrier, inc=1, device_id=ring_device(offset), device_id_type=MESH)
    for offset in (1, Y - 1):
        pl.semaphore_signal(barrier, inc=1, device_id=cross_device(offset), device_id_type=MESH)

    table_ref[...] = transform_table()
    kept[...] = jnp.zeros_like(kept)
    kept[0:4, 0:STA] = flag_ref[...]
    square[...] = jnp.zeros_like(square)
    square[0:8, :] = kept[...]
    words = jnp.transpose(square[...])[0:STA]
    lane = lax.broadcasted_iota(jnp.int32, (STA, WIN), 1)
    spread = jnp.broadcast_to(words[:, 0:1], (STA, WIN))
    for j in range(1, 4):
        spread = jnp.where(lane >= 32 * j, jnp.broadcast_to(words[:, j : j + 1], (STA, WIN)), spread)
    usable[...] = (lax.shift_right_logical(spread, lane % 32) & 1).astype(jnp.float32)
    low = lax.broadcasted_iota(jnp.int32, (1, WIN), 1) < STA
    rows = kept[...]
    rolled = pltpu.roll(rows, STA, 1)
    word_ref[0:1] = jnp.where(low, rows[0:1], rolled[1:2])
    word_ref[1:2] = jnp.where(low, rows[2:3], rolled[3:4])

    def transform(q):
        def pair(n, carry):
            first = PART * q + STEP * n
            both = rec[pl.ds(first, STEP)].reshape(STEP * WIN, LEN)
            spectrum = lax.dot_general(table_ref[...], both, NT, preferred_element_type=jnp.float32)
            for s in range(STEP):
                re = [spectrum[8 * v : 8 * v + 8, WIN * s : WIN * (s + 1)] for v in range(5)]
                im = [spectrum[SLOTS + 8 * v : SLOTS + 8 * v + 8, WIN * s : WIN * (s + 1)] for v in range(5)]
                m = [jnp.sqrt(a * a + b * b) for a, b in zip(re, im)]

                def above(x):
                    return pltpu.roll(x, 7, 0)

                def below(x):
                    return pltpu.roll(x, 1, 0)

                low, high = m[0] + m[1], m[3] + m[4]
                sums = [
                    low + m[2] + below(high),
                    low + m[2] + m[3] + below(m[4]),
                    low + m[2] + high,
                    m[1] + m[2] + high + above(m[0]),
                    m[2] + high + above(low),
                ]
                keep = jnp.broadcast_to(usable[pl.ds(first + s, 1), :], (8, WIN))
                for v in range(5):
                    factor = keep / jnp.maximum(sums[v] * 0.2, FLOOR)
                    at = pl.multiple_of((STEP * n + s) * SLOTS + 8 * v, 8)
                    stage_re[pl.ds(at, 8), :] = re[v] * factor
                    stage_im[pl.ds(at, 8), :] = im[v] * factor
            return carry

        lax.fori_loop(0, PART // STEP, pair, 0)
        for p in range(PLANE):
            i, v = (p + 2) // 5, (p + 2) % 5
            for half, stage in ((0, stage_re), (1, stage_im)):
                rows = stage[pl.ds(8 * v + i, PART, stride=SLOTS), :]
                spec[p, PART * q : PART * (q + 1), WIN * half : WIN * (half + 1)] = rows.astype(jnp.bfloat16)

    def plane_copy(q, sender, receiver):
        at = pl.ds(PART * q, PART)
        return pltpu.make_async_remote_copy(
            spec.at[receiver, at, :], gathered.at[y, sender % 2, sender // 2, at, :],
            plane_send.at[q, receiver], plane_recv.at[q, sender],
            device_id=plane_device(receiver), device_id_type=MESH)

    def group_peer(step, j):
        return 8 * ((x + step) % 4) + (spot + j) % 8

    def send_plane(q):
        for step in NEAR:
            for j in range(0 if step else 1, 8):
                plane_copy(q, mine, group_peer(step, j)).start()
        gathered[y, zl, freq, PART * q : PART * (q + 1), :] = spec[mine, PART * q : PART * (q + 1), :]

    def from_plane(q, step):
        for j in range(0 if step else 1, 8):
            sender = group_peer(step, j)
            plane_copy(q, sender, (sender + 1) % PLANE).wait_recv()

    for q in range(CHUNKS):
        loads[q].wait()
        if q == 0:
            for copy in loads[1:]:
                copy.start()
        transform(q)
        if q == 0:
            pl.semaphore_wait(barrier, PLANE - 1 + Y - 1 + 2)
        send_plane(q)

    ring_words[y] = word_ref[...]
    word_ring = [
        pltpu.make_async_remote_copy(
            word_ref, ring_words.at[y], wring_send.at[offset], wring_recv.at[offset],
            device_id=ring_device(offset), device_id_type=MESH)
        for offset in range(1, Y)
    ]
    for copy in word_ring:
        copy.start()

    def message(entry, slot, step, send, recv):
        kind, shift, (how, n) = entry
        owner = y if kind == "own" else (y - step + Y) % Y
        group = 4 * ((owner + shift) % Y)
        if how == "q":
            ref = gathered.at[owner, :, pl.ds(group, 4), pl.ds(PART * n, PART), :]
        else:
            ref = gathered.at[owner, :, pl.ds(group + 2 * n, 2), :, :]
        return pltpu.make_async_remote_copy(
            ref, ref, send.at[slot], recv.at[slot],
            device_id=ring_device(step % Y), device_id_type=MESH)

    ups = [message(entry, slot, 1, up_send, up_recv) for slot, entry in enumerate(UP)]
    downs = [message(entry, slot, -1, down_send, down_recv) for slot, entry in enumerate(DOWN)]

    def ring_start(q, step):
        group = (x + step) % 4
        shift = (group - y + Y) % Y
        ref = gathered.at[y, :, pl.ds(4 * group, 4), pl.ds(PART * q, PART), :]
        upward = (shift + 1) // 2 == 1

        @pl.when(upward)
        def _():
            slot = CHUNKS * (shift - 1) + q
            pltpu.make_async_remote_copy(
                ref, ref, up_send.at[slot], up_recv.at[slot],
                device_id=ring_device(1), device_id_type=MESH).start()

        @pl.when(jnp.logical_not(upward))
        def _():
            slot = CHUNKS * ((3 - shift) // 3) + q
            pltpu.make_async_remote_copy(
                ref, ref, down_send.at[slot], down_recv.at[slot],
                device_id=ring_device(Y - 1), device_id_type=MESH).start()

    for q in range(CHUNKS):
        for step in NEAR:
            from_plane(q, step)
            ring_start(q, step)
        if q == 0:
            for copy in word_ring:
                copy.wait()

            def word_copy(sender, receiver):
                return pltpu.make_async_remote_copy(
                    ring_words, all_words.at[sender],
                    wplane_send.at[receiver], wplane_recv.at[sender],
                    device_id=plane_device(receiver), device_id_type=MESH)

            def send_words(offset, carry):
                word_copy(mine, (mine + offset) % PLANE).start()
                return carry

            lax.fori_loop(1, PLANE, send_words, 0)
            all_words[mine] = ring_words[...]

    for q in range(CHUNKS):
        ups[4 + q].wait_recv()
        ups[8 + q].start()
        downs[q].wait_recv()
        downs[8 + q].start()
    ups[12].start()
    downs[12].start()
    ups[13].start()
    for q in range(CHUNKS):
        downs[4 + q].wait_recv()
    downs[13].start()
    downs[14].start()
    downs[15].start()

    def words_here(offset, carry):
        sender = (mine + offset) % PLANE
        word_copy(sender, sender).wait_recv()
        return carry

    lax.fori_loop(1, PLANE, words_here, 0)
    lane2 = lax.broadcasted_iota(jnp.int32, (2, WIN), 1)
    for owner in range(Y):
        for part in range(2):
            base = 4 * (2 * owner + part)
            for g in range(8):
                a = all_words[4 * g + part, owner]
                b = all_words[4 * g + 2 + part, owner]
                flat_words[base : base + 2, WIN * g : WIN * (g + 1)] = jnp.where(
                    lane2 < 64, a, pltpu.roll(b, 64, 1))
                flat_words[base + 2 : base + 4, WIN * g : WIN * (g + 1)] = jnp.where(
                    lane2 < 64, pltpu.roll(a, 64, 1), b)
    shifts = lax.broadcasted_iota(jnp.int32, (32, 1024), 0)

    def unpack(n, carry):
        row = jnp.broadcast_to(flat_words[pl.ds(n, 1), :], (32, 1024))
        bit = (lax.shift_right_logical(row, shifts) & 1).astype(jnp.float32)
        bits[pl.ds(pl.multiple_of(32 * n, 32), 32), :] = bit.astype(jnp.bfloat16)
        return carry

    lax.fori_loop(0, 32, unpack, 0)
    here = bits[:, pl.ds(pl.multiple_of(y * ROWS, ROWS), ROWS)]
    counts = lax.dot_general(here, bits[...], TN, preferred_element_type=jnp.float32)
    inverse[...] = 1.0 / jnp.maximum(counts, 1.0)
    kept_at = pl.multiple_of(zl * SIDE, SIDE)
    away_at = pl.multiple_of((1 - zl) * SIDE, SIDE)

    def encode(values):
        top = jnp.maximum(jnp.max(jnp.abs(values), axis=0, keepdims=True), 1e-30)
        codes = jnp.round(values * (32767.0 / top)).astype(jnp.int32).astype(jnp.int16)
        return codes, top / 32767.0

    def decode(codes, scale):
        return codes.astype(jnp.int32).astype(jnp.float32) * scale

    def swap(shift, slot, at, width):
        for plane in range(2):
            side_out[shift, plane, :, at], side_scale_out[slot, plane : plane + 1, 0:width] = encode(
                block[shift, plane, pl.ds(away_at, SIDE), at])
        copies = [
            pltpu.make_async_remote_copy(
                source, target, side_send.at[kind, slot], side_recv.at[kind, slot],
                device_id=(2 * y + 1 - zl, freq), device_id_type=MESH)
            for kind, (source, target) in enumerate((
                (side_scale_out.at[slot], side_scale_in.at[slot]),
                (side_out.at[shift, :, :, at], side_in.at[shift, :, :, at])))
        ]
        for copy in copies:
            copy.start()
        return copies

    def right_side(group, count, first, last):
        return jnp.concatenate(
            [gathered[(y + k) % Y, part, pl.ds(group, count)].reshape(STA * count, 2 * WIN)
             for k in OWNERS[first:last] for part in range(2)], axis=1)

    def multiply(shift):
        both = lax.dot_general(
            turned[:, 1536:2048], right_side(4 * ((y + shift) % Y), 4, 3, 4), NT,
            preferred_element_type=jnp.float32)
        col = pl.multiple_of(((y + shift) % Y) * ROWS, ROWS)
        block[shift] = (block[shift] + both.reshape(2, ROWS, ROWS)) * inverse[:, pl.ds(col, ROWS)]
        copies = swap(shift, shift, slice(0, ROWS), ROWS)
        out_ref[zl, :, :, pl.ds(col, ROWS)] = block[shift, :, pl.ds(kept_at, SIDE), :]
        return copies

    def multiply_late(half, late):
        group = 4 * ((y + 2) % Y) + 2 * half
        at = slice(SIDE * half, SIDE * (half + 1))
        col = pl.multiple_of(group * STA, SIDE)
        early = lax.dot_general(
            turned[:, 0:1536], right_side(group, 2, 0, 3), NT, preferred_element_type=jnp.float32)
        block[2, :, :, at] = early.reshape(2, ROWS, SIDE)
        late.wait_recv()
        right = right_side(group, 2, 3, 4)

        def finish(rows):
            left = jnp.concatenate(
                [turned[pl.ds(rows + start, SIDE), 1536:2048] for start in (0, ROWS)], axis=0)
            both = lax.dot_general(left, right, NT, preferred_element_type=jnp.float32)
            block[2, :, pl.ds(rows, SIDE), at] = (
                block[2, :, pl.ds(rows, SIDE), at] + both.reshape(2, SIDE, SIDE)
            ) * inverse[pl.ds(rows, SIDE), pl.ds(col, SIDE)]

        finish(away_at)
        copies = swap(2, 2 + half, at, SIDE)
        finish(kept_at)
        out_ref[zl, :, :, pl.ds(col, SIDE)] = block[2, :, pl.ds(kept_at, SIDE), at]
        return copies

    def left_side(n):
        for part in range(2):
            left = gathered[(y + OWNERS[n]) % Y, part, pl.ds(4 * y, 4)].reshape(ROWS, 2 * WIN)
            at = (2 * n + part) * 256
            turned[0:ROWS, at : at + 256] = left
            turned[ROWS : 2 * ROWS, at : at + 256] = jnp.concatenate(
                [left[:, WIN:], -left[:, :WIN]], axis=1)

    for q in range(CHUNKS):
        ups[q].wait_recv()
    for n in range(3):
        left_side(n)
    for shift in (1, 0):
        early = lax.dot_general(
            turned[:, 0:1536], right_side(4 * ((y + shift) % Y), 4, 0, 3), NT,
            preferred_element_type=jnp.float32)
        block[shift] = early.reshape(2, ROWS, ROWS)
    for q in range(CHUNKS):
        ups[8 + q].wait_recv()
        downs[8 + q].wait_recv()
    left_side(3)
    sides = [multiply(1), multiply(0)]
    for plane, sign in ((0, 1.0), (1, -1.0)):
        flipped = sign * jnp.transpose(block[1, plane])
        for h in range(2):
            mirror_out[h, plane], mirror_scale_out[h, plane : plane + 1] = encode(
                flipped[SIDE * h : SIDE * (h + 1)])
    mirrors = [
        pltpu.make_async_remote_copy(
            source.at[part], target.at[zl],
            mirror_send.at[kind, n], mirror_recv.at[kind, n], device_id=device, device_id_type=MESH)
        for n, (part, device) in enumerate(((zl, ring_device(1)), (1 - zl, cross_device(1))))
        for kind, (source, target) in enumerate(
            ((mirror_scale_out, mirror_scale_in), (mirror_out, mirror_in)))
    ]
    for copy in mirrors:
        copy.start()
    ups[12].wait_recv()
    downs[12].wait_recv()
    sides.append(multiply_late(0, downs[13]))
    ups[13].wait_recv()
    downs[14].wait_recv()
    sides.append(multiply_late(1, downs[15]))

    def column(shift, half=None):
        if half is None:
            return pl.ds(pl.multiple_of(((y + shift) % Y) * ROWS, ROWS), ROWS)
        return pl.ds(pl.multiple_of(((y + shift) % Y) * ROWS + SIDE * half, SIDE), SIDE)

    for shift in (1, 0):
        for copy in sides[1 - shift]:
            copy.wait()
        for plane in range(2):
            out_ref[1 - zl, plane, :, column(shift)] = decode(
                side_in[shift, plane], side_scale_in[shift, plane : plane + 1])
    for copy in mirrors:
        copy.wait()
    for n in range(2):
        for plane in range(2):
            out_ref[n, plane, :, column(3)] = decode(
                mirror_in[n, plane], mirror_scale_in[n, plane : plane + 1])

    def sent(offset, carry):
        other = (mine + offset) % PLANE
        for q in range(CHUNKS):
            plane_copy(q, mine, other).wait_send()
        word_copy(mine, other).wait_send()
        return carry

    lax.fori_loop(1, PLANE, sent, 0)
    for copy in ups + downs:
        copy.wait_send()
    for half in range(2):
        for copy in sides[2 + half]:
            copy.wait()
        for plane in range(2):
            out_ref[1 - zl, plane, :, column(2, half)] = decode(
                side_in[2, plane, :, SIDE * half : SIDE * (half + 1)],
                side_scale_in[2 + half, plane : plane + 1, 0:SIDE])


def stack_up(records, flags):
    dma = pltpu.SemaphoreType.DMA
    vmem = pl.BlockSpec(memory_space=pltpu.VMEM)
    return pl.pallas_call(
        kernel,
        out_shape=jax.ShapeDtypeStruct((2, 2, SIDE, 1024), jnp.float32),
        in_specs=[pl.BlockSpec(memory_space=pl.ANY), vmem],
        out_specs=vmem,
        scratch_shapes=[
            pltpu.VMEM((STA, WIN, LEN), jnp.bfloat16),
            pltpu.VMEM((2 * SLOTS, LEN), jnp.bfloat16),
            pltpu.VMEM((8, WIN), jnp.int32),
            pltpu.VMEM((WIN, WIN), jnp.int32),
            pltpu.VMEM((2, WIN), jnp.int32),
            pltpu.VMEM((STA, WIN), jnp.float32),
            pltpu.VMEM((PART * SLOTS, WIN), jnp.float32),
            pltpu.VMEM((PART * SLOTS, WIN), jnp.float32),
            pltpu.VMEM((PLANE, STA, 2 * WIN), jnp.bfloat16),
            pltpu.VMEM((Y, 2, 16, STA, 2 * WIN), jnp.bfloat16),
            pltpu.VMEM((2 * ROWS, 2048), jnp.bfloat16),
            pltpu.VMEM((3, 2, ROWS, ROWS), jnp.float32),
            pltpu.VMEM((Y, 2, WIN), jnp.int32),
            pltpu.VMEM((PLANE, Y, 2, WIN), jnp.int32),
            pltpu.VMEM((PLANE, 1024), jnp.int32),
            pltpu.VMEM((1024, 1024), jnp.bfloat16),
            pltpu.VMEM((ROWS, 1024), jnp.float32),
            pltpu.VMEM((3, 2, SIDE, ROWS), jnp.int16),
            pltpu.VMEM((3, 2, SIDE, ROWS), jnp.int16),
            pltpu.VMEM((2, 2, SIDE, ROWS), jnp.int16),
            pltpu.VMEM((2, 2, SIDE, ROWS), jnp.int16),
            pltpu.VMEM((4, 2, ROWS), jnp.float32),
            pltpu.VMEM((4, 2, ROWS), jnp.float32),
            pltpu.VMEM((2, 2, ROWS), jnp.float32),
            pltpu.VMEM((2, 2, ROWS), jnp.float32),
            dma((CHUNKS,)), dma((CHUNKS, PLANE)), dma((CHUNKS, PLANE)),
            dma((Y,)), dma((Y,)), dma((PLANE,)), dma((PLANE,)),
            dma((len(UP),)), dma((len(UP),)), dma((len(DOWN),)), dma((len(DOWN),)),
            dma((2, 4)), dma((2, 4)), dma((2, 2)), dma((2, 2)),
        ],
        compiler_params=pltpu.CompilerParams(
            collective_id=0, has_side_effects=True, vmem_limit_bytes=48 << 20),
    )(records, flags)


def local(records, gap_flags, station_mask):
    return stack_up(records, gap_flags.T * station_mask[None])


def solution(mesh):
    placed = (P("freq", "tm", None), P("freq", "tm"), P("freq"))
    return jax.shard_map(
        local, mesh=mesh, in_specs=placed, out_specs=P("freq", None, "tm", None), check_vma=False
    )
```

```python
import math

import jax
import jax.numpy as jnp
from jax import lax
from jax.experimental import pallas as pl
from jax.experimental.pallas import tpu as pltpu
from jax.sharding import PartitionSpec as P

FLOOR = 0.25
MESH = pl.DeviceIdType.MESH
Y = 4
PLANE = 32
STA = 64
CHUNKS = 4
PART = STA // CHUNKS
WIN = 128
LEN = 512
ROWS = 256
SIDE = 128
STEP = 8
SLOTS = 40
NEAR = (0, 1, 3, 2)
OWNERS = (0, 1, 3, 2)
NT = (((1,), (1,)), ((), ()))
TN = (((0,), (0,)), ((), ()))
QUARTERS = tuple(("q", q) for q in range(CHUNKS))
FIRST, SECOND = ("h", 0), ("h", 1)
UP = (
    [("own", 1, q) for q in QUARTERS]
    + [("own", 2, q) for q in QUARTERS]
    + [("fwd", 2, q) for q in QUARTERS]
    + [("own", 3, FIRST), ("own", 3, SECOND)]
)
DOWN = (
    [("own", 3, q) for q in QUARTERS]
    + [("own", 0, q) for q in QUARTERS]
    + [("fwd", 3, q) for q in QUARTERS]
    + [("own", 1, FIRST), ("fwd", 0, FIRST), ("own", 1, SECOND), ("fwd", 0, SECOND)]
)


def turn(phase):
    quarter = (phase + 64) // 128
    a = (phase - 128 * quarter).astype(jnp.float32) * (2.0 * math.pi / LEN)
    b = a * a
    c = 1.0 + b * (-0.5 + b * (1.0 / 24 + b * (-1.0 / 720 + b * (1.0 / 40320))))
    s = a * (1.0 + b * (-1.0 / 6 + b * (1.0 / 120 + b * (-1.0 / 5040 + b * (1.0 / 362880)))))
    odd = quarter % 2 == 1
    cosine = jnp.where(odd, s, c)
    sine = jnp.where(odd, c, s)
    cosine = jnp.where((quarter == 1) | (quarter == 2), -cosine, cosine)
    sine = jnp.where((quarter == 2) | (quarter == 3), -sine, sine)
    return cosine, sine


def transform_table():
    row = lax.broadcasted_iota(jnp.int32, (SLOTS, LEN), 0)
    t = lax.broadcasted_iota(jnp.int32, (SLOTS, LEN), 1)
    b = 5 * (row % 8) + row // 8
    taper = jnp.where(b < 36, (0.5 - 0.5 * turn(t)[0]) * (1.0 / math.sqrt(LEN)), 0.0)
    cosine, sine = turn((b * t) % LEN)
    return jnp.concatenate([cosine * taper, -sine * taper], axis=0).astype(jnp.bfloat16)


def kernel(
    rec_hbm, flag_ref, out_ref,
    rec, table_ref, kept, square, word_ref, usable, stage_re, stage_im, spec, gathered, turned, block,
    ring_words, all_words, flat_words, bits, inverse, side_out, side_in, mirror_out, mirror_in,
    side_scale_out, side_scale_in, mirror_scale_out, mirror_scale_in,
    rec_sem, plane_send, plane_recv, wring_send, wring_recv, wplane_send, wplane_recv,
    up_send, up_recv, down_send, down_recv, side_send, side_recv, mirror_send, mirror_recv,
):
    tm = lax.axis_index("tm")
    freq = lax.axis_index("freq")
    y, zl = tm // 2, tm % 2
    mine = 2 * freq + zl
    x, spot = mine // 8, mine % 8

    def plane_device(other):
        return (2 * y + other % 2, other // 2)

    def ring_device(offset):
        return (2 * ((y + offset) % Y) + zl, freq)

    def cross_device(offset):
        return (2 * ((y + offset) % Y) + 1 - zl, freq)

    loads = [
        pltpu.make_async_copy(
            rec_hbm.at[pl.ds(PART * q, PART)], rec.at[pl.ds(PART * q, PART)], rec_sem.at[q])
        for q in range(CHUNKS)
    ]
    loads[0].start()

    barrier = pltpu.get_barrier_semaphore()

    def greet(offset, carry):
        pl.semaphore_signal(
            barrier, inc=1, device_id=plane_device((mine + offset) % PLANE), device_id_type=MESH)
        return carry

    for offset in range(1, PLANE):
        greet(offset, 0)
    for offset in range(1, Y):
        pl.semaphore_signal(barrier, inc=1, device_id=ring_device(offset), device_id_type=MESH)
    for offset in (1, Y - 1):
        pl.semaphore_signal(barrier, inc=1, device_id=cross_device(offset), device_id_type=MESH)

    table_ref[...] = transform_table()
    kept[...] = jnp.zeros_like(kept)
    kept[0:4, 0:STA] = flag_ref[...]
    square[...] = jnp.zeros_like(square)
    square[0:8, :] = kept[...]
    words = jnp.transpose(square[...])[0:STA]
    lane = lax.broadcasted_iota(jnp.int32, (STA, WIN), 1)
    spread = jnp.broadcast_to(words[:, 0:1], (STA, WIN))
    for j in range(1, 4):
        spread = jnp.where(lane >= 32 * j, jnp.broadcast_to(words[:, j : j + 1], (STA, WIN)), spread)
    usable[...] = (lax.shift_right_logical(spread, lane % 32) & 1).astype(jnp.float32)
    low = lax.broadcasted_iota(jnp.int32, (1, WIN), 1) < STA
    rows = kept[...]
    rolled = pltpu.roll(rows, STA, 1)
    word_ref[0:1] = jnp.where(low, rows[0:1], rolled[1:2])
    word_ref[1:2] = jnp.where(low, rows[2:3], rolled[3:4])

    def transform(q):
        def pair(n, carry):
            first = PART * q + STEP * n
            both = rec[pl.ds(first, STEP)].reshape(STEP * WIN, LEN)
            spectrum = lax.dot_general(table_ref[...], both, NT, preferred_element_type=jnp.float32)
            for s in range(STEP):
                re = [spectrum[8 * v : 8 * v + 8, WIN * s : WIN * (s + 1)] for v in range(5)]
                im = [spectrum[SLOTS + 8 * v : SLOTS + 8 * v + 8, WIN * s : WIN * (s + 1)] for v in range(5)]
                m = [jnp.sqrt(a * a + b * b) for a, b in zip(re, im)]

                def above(x):
                    return pltpu.roll(x, 7, 0)

                def below(x):
                    return pltpu.roll(x, 1, 0)

                low, high = m[0] + m[1], m[3] + m[4]
                sums = [
                    low + m[2] + below(high),
                    low + m[2] + m[3] + below(m[4]),
                    low + m[2] + high,
                    m[1] + m[2] + high + above(m[0]),
                    m[2] + high + above(low),
                ]
                keep = jnp.broadcast_to(usable[pl.ds(first + s, 1), :], (8, WIN))
                for v in range(5):
                    factor = keep / jnp.maximum(sums[v] * 0.2, FLOOR)
                    at = pl.multiple_of((STEP * n + s) * SLOTS + 8 * v, 8)
                    stage_re[pl.ds(at, 8), :] = re[v] * factor
                    stage_im[pl.ds(at, 8), :] = im[v] * factor
            return carry

        lax.fori_loop(0, PART // STEP, pair, 0)
        for p in range(PLANE):
            i, v = (p + 2) // 5, (p + 2) % 5
            for half, stage in ((0, stage_re), (1, stage_im)):
                rows = stage[pl.ds(8 * v + i, PART, stride=SLOTS), :]
                spec[p, PART * q : PART * (q + 1), WIN * half : WIN * (half + 1)] = rows.astype(jnp.bfloat16)

    def plane_copy(q, sender, receiver):
        at = pl.ds(PART * q, PART)
        return pltpu.make_async_remote_copy(
            spec.at[receiver, at, :], gathered.at[y, sender % 2, sender // 2, at, :],
            plane_send.at[q, receiver], plane_recv.at[q, sender],
            device_id=plane_device(receiver), device_id_type=MESH)

    def group_peer(step, j):
        return 8 * ((x + step) % 4) + (spot + j) % 8

    def send_plane(q):
        for step in NEAR:
            for j in range(0 if step else 1, 8):
                plane_copy(q, mine, group_peer(step, j)).start()
        gathered[y, zl, freq, PART * q : PART * (q + 1), :] = spec[mine, PART * q : PART * (q + 1), :]

    def from_plane(q, step):
        for j in range(0 if step else 1, 8):
            sender = group_peer(step, j)
            plane_copy(q, sender, (sender + 1) % PLANE).wait_recv()

    for q in range(CHUNKS):
        loads[q].wait()
        if q == 0:
            for copy in loads[1:]:
                copy.start()
        transform(q)
        if q == 0:
            pl.semaphore_wait(barrier, PLANE - 1 + Y - 1 + 2)
        send_plane(q)

    ring_words[y] = word_ref[...]
    word_ring = [
        pltpu.make_async_remote_copy(
            word_ref, ring_words.at[y], wring_send.at[offset], wring_recv.at[offset],
            device_id=ring_device(offset), device_id_type=MESH)
        for offset in range(1, Y)
    ]
    for copy in word_ring:
        copy.start()

    def message(entry, slot, step, send, recv):
        kind, shift, (how, n) = entry
        owner = y if kind == "own" else (y - step + Y) % Y
        group = 4 * ((owner + shift) % Y)
        if how == "q":
            ref = gathered.at[owner, :, pl.ds(group, 4), pl.ds(PART * n, PART), :]
        else:
            ref = gathered.at[owner, :, pl.ds(group + 2 * n, 2), :, :]
        return pltpu.make_async_remote_copy(
            ref, ref, send.at[slot], recv.at[slot],
            device_id=ring_device(step % Y), device_id_type=MESH)

    ups = [message(entry, slot, 1, up_send, up_recv) for slot, entry in enumerate(UP)]
    downs = [message(entry, slot, -1, down_send, down_recv) for slot, entry in enumerate(DOWN)]

    def ring_start(q, step):
        group = (x + step) % 4
        shift = (group - y + Y) % Y
        ref = gathered.at[y, :, pl.ds(4 * group, 4), pl.ds(PART * q, PART), :]
        upward = (shift + 1) // 2 == 1

        @pl.when(upward)
        def _():
            slot = CHUNKS * (shift - 1) + q
            pltpu.make_async_remote_copy(
                ref, ref, up_send.at[slot], up_recv.at[slot],
                device_id=ring_device(1), device_id_type=MESH).start()

        @pl.when(jnp.logical_not(upward))
        def _():
            slot = CHUNKS * ((3 - shift) // 3) + q
            pltpu.make_async_remote_copy(
                ref, ref, down_send.at[slot], down_recv.at[slot],
                device_id=ring_device(Y - 1), device_id_type=MESH).start()

    for q in range(CHUNKS):
        for step in NEAR:
            from_plane(q, step)
            ring_start(q, step)
        if q == 0:
            for copy in word_ring:
                copy.wait()

            def word_copy(sender, receiver):
                return pltpu.make_async_remote_copy(
                    ring_words, all_words.at[sender],
                    wplane_send.at[receiver], wplane_recv.at[sender],
                    device_id=plane_device(receiver), device_id_type=MESH)

            def send_words(offset, carry):
                word_copy(mine, (mine + offset) % PLANE).start()
                return carry

            lax.fori_loop(1, PLANE, send_words, 0)
            all_words[mine] = ring_words[...]

    for q in range(CHUNKS):
        ups[4 + q].wait_recv()
        ups[8 + q].start()
        downs[q].wait_recv()
        downs[8 + q].start()
    ups[12].start()
    downs[12].start()
    ups[13].start()
    for q in range(CHUNKS):
        downs[4 + q].wait_recv()
    downs[13].start()
    downs[14].start()
    downs[15].start()

    def words_here(offset, carry):
        sender = (mine + offset) % PLANE
        word_copy(sender, sender).wait_recv()
        return carry

    lax.fori_loop(1, PLANE, words_here, 0)
    lane2 = lax.broadcasted_iota(jnp.int32, (2, WIN), 1)
    for owner in range(Y):
        for part in range(2):
            base = 4 * (2 * owner + part)
            for g in range(8):
                a = all_words[4 * g + part, owner]
                b = all_words[4 * g + 2 + part, owner]
                flat_words[base : base + 2, WIN * g : WIN * (g + 1)] = jnp.where(
                    lane2 < 64, a, pltpu.roll(b, 64, 1))
                flat_words[base + 2 : base + 4, WIN * g : WIN * (g + 1)] = jnp.where(
                    lane2 < 64, pltpu.roll(a, 64, 1), b)
    shifts = lax.broadcasted_iota(jnp.int32, (32, 1024), 0)

    def unpack(n, carry):
        row = jnp.broadcast_to(flat_words[pl.ds(n, 1), :], (32, 1024))
        bit = (lax.shift_right_logical(row, shifts) & 1).astype(jnp.float32)
        bits[pl.ds(pl.multiple_of(32 * n, 32), 32), :] = bit.astype(jnp.bfloat16)
        return carry

    lax.fori_loop(0, 32, unpack, 0)
    here = bits[:, pl.ds(pl.multiple_of(y * ROWS, ROWS), ROWS)]
    counts = lax.dot_general(here, bits[...], TN, preferred_element_type=jnp.float32)
    inverse[...] = 1.0 / jnp.maximum(counts, 1.0)
    kept_at = pl.multiple_of(zl * SIDE, SIDE)
    away_at = pl.multiple_of((1 - zl) * SIDE, SIDE)

    def encode(values):
        top = jnp.maximum(jnp.max(jnp.abs(values), axis=0, keepdims=True), 1e-30)
        codes = jnp.round(values * (32767.0 / top)).astype(jnp.int32).astype(jnp.int16)
        return codes, top / 32767.0

    def decode(codes, scale):
        return codes.astype(jnp.int32).astype(jnp.float32) * scale

    def side_copy(source, target, kind, slot):
        return pltpu.make_async_remote_copy(
            source, target, side_send.at[kind, slot], side_recv.at[kind, slot],
            device_id=(2 * y + 1 - zl, freq), device_id_type=MESH)

    def start(pairs, slot):
        for kind in range(0 if len(pairs) == 1 else 1, len(pairs)):
            side_copy(*pairs[kind], kind, slot).start()

    def swap(shift, slot, at, width):
        for plane in range(2):
            side_out[shift, plane, :, at], side_scale_out[slot, plane : plane + 1, 0:width] = encode(
                block[shift, plane, pl.ds(away_at, SIDE), at])
        copies = [
            pltpu.make_async_remote_copy(
                source, target, side_send.at[kind, slot], side_recv.at[kind, slot],
                device_id=(2 * y + 1 - zl, freq), device_id_type=MESH)
            for kind, (source, target) in enumerate((
                (side_scale_out.at[slot], side_scale_in.at[slot]),
                (side_out.at[shift, :, :, at], side_in.at[shift, :, :, at])))
        ]
        for copy in copies:
            copy.start()
        return copies

    def right_side(group, count, first, last):
        return jnp.concatenate(
            [gathered[(y + k) % Y, part, pl.ds(group, count)].reshape(STA * count, 2 * WIN)
             for k in OWNERS[first:last] for part in range(2)], axis=1)

    def multiply(shift):
        both = lax.dot_general(
            turned[:, 1536:2048], right_side(4 * ((y + shift) % Y), 4, 3, 4), NT,
            preferred_element_type=jnp.float32)
        col = pl.multiple_of(((y + shift) % Y) * ROWS, ROWS)
        block[shift] = (block[shift] + both.reshape(2, ROWS, ROWS)) * inverse[:, pl.ds(col, ROWS)]
        copies = swap(shift, shift, slice(0, ROWS), ROWS)
        out_ref[zl, :, :, pl.ds(col, ROWS)] = block[shift, :, pl.ds(kept_at, SIDE), :]
        return copies

    def multiply_late(half, late):
        group = 4 * ((y + 2) % Y) + 2 * half
        at = slice(SIDE * half, SIDE * (half + 1))
        col = pl.multiple_of(group * STA, SIDE)
        early = lax.dot_general(
            turned[:, 0:1536], right_side(group, 2, 0, 3), NT, preferred_element_type=jnp.float32)
        block[2, :, :, at] = early.reshape(2, ROWS, SIDE)
        late.wait_recv()
        right = right_side(group, 2, 3, 4)

        def finish(rows, plane):
            both = lax.dot_general(
                turned[pl.ds(rows + ROWS * plane, SIDE), 1536:2048], right, NT,
                preferred_element_type=jnp.float32)
            return (block[2, plane, pl.ds(rows, SIDE), at] + both) * inverse[pl.ds(rows, SIDE), pl.ds(col, SIDE)]

        slot = 2 + half
        pairs = []
        for plane in range(2):
            side_out[2, plane, :, at], side_scale_out[slot, plane : plane + 1, 0:SIDE] = encode(
                finish(away_at, plane))
            pairs.append((side_out.at[2, plane, :, at], side_in.at[2, plane, :, at]))
            if plane == 1:
                pairs.append((side_scale_out.at[slot], side_scale_in.at[slot]))
                start(pairs, slot)
            else:
                start(pairs, slot)
        for plane in range(2):
            out_ref[zl, plane, :, pl.ds(col, SIDE)] = finish(kept_at, plane)
        return [side_copy(source, target, kind, slot) for kind, (source, target) in enumerate(pairs)]

    def left_side(n):
        for part in range(2):
            left = gathered[(y + OWNERS[n]) % Y, part, pl.ds(4 * y, 4)].reshape(ROWS, 2 * WIN)
            at = (2 * n + part) * 256
            turned[0:ROWS, at : at + 256] = left
            turned[ROWS : 2 * ROWS, at : at + 256] = jnp.concatenate(
                [left[:, WIN:], -left[:, :WIN]], axis=1)

    for q in range(CHUNKS):
        ups[q].wait_recv()
    for n in range(3):
        left_side(n)
    for shift in (1, 0):
        early = lax.dot_general(
            turned[:, 0:1536], right_side(4 * ((y + shift) % Y), 4, 0, 3), NT,
            preferred_element_type=jnp.float32)
        block[shift] = early.reshape(2, ROWS, ROWS)
    for q in range(CHUNKS):
        ups[8 + q].wait_recv()
        downs[8 + q].wait_recv()
    left_side(3)
    sides = [multiply(1), multiply(0)]
    for plane, sign in ((0, 1.0), (1, -1.0)):
        flipped = sign * jnp.transpose(block[1, plane])
        for h in range(2):
            mirror_out[h, plane], mirror_scale_out[h, plane : plane + 1] = encode(
                flipped[SIDE * h : SIDE * (h + 1)])
    mirrors = [
        pltpu.make_async_remote_copy(
            source.at[part], target.at[zl],
            mirror_send.at[kind, n], mirror_recv.at[kind, n], device_id=device, device_id_type=MESH)
        for n, (part, device) in enumerate(((1 - zl, cross_device(1)), (zl, ring_device(1))))
        for kind, (source, target) in enumerate(
            ((mirror_scale_out, mirror_scale_in), (mirror_out, mirror_in)))
    ]
    for copy in mirrors:
        copy.start()
    ups[12].wait_recv()
    downs[12].wait_recv()
    sides.append(multiply_late(0, downs[13]))
    ups[13].wait_recv()
    downs[14].wait_recv()
    sides.append(multiply_late(1, downs[15]))

    def column(shift, half=None):
        if half is None:
            return pl.ds(pl.multiple_of(((y + shift) % Y) * ROWS, ROWS), ROWS)
        return pl.ds(pl.multiple_of(((y + shift) % Y) * ROWS + SIDE * half, SIDE), SIDE)

    for shift in (1, 0):
        for copy in sides[1 - shift]:
            copy.wait()
        for plane in range(2):
            out_ref[1 - zl, plane, :, column(shift)] = decode(
                side_in[shift, plane], side_scale_in[shift, plane : plane + 1])
    for copy in mirrors:
        copy.wait()
    for n in range(2):
        for plane in range(2):
            out_ref[n, plane, :, column(3)] = decode(
                mirror_in[n, plane], mirror_scale_in[n, plane : plane + 1])

    def sent(offset, carry):
        other = (mine + offset) % PLANE
        for q in range(CHUNKS):
            plane_copy(q, mine, other).wait_send()
        word_copy(mine, other).wait_send()
        return carry

    lax.fori_loop(1, PLANE, sent, 0)
    for copy in ups + downs:
        copy.wait_send()
    for half in range(2):
        for copy in sides[2 + half]:
            copy.wait()
        for plane in range(2):
            out_ref[1 - zl, plane, :, column(2, half)] = decode(
                side_in[2, plane, :, SIDE * half : SIDE * (half + 1)],
                side_scale_in[2 + half, plane : plane + 1, 0:SIDE])


def stack_up(records, flags):
    dma = pltpu.SemaphoreType.DMA
    vmem = pl.BlockSpec(memory_space=pltpu.VMEM)
    return pl.pallas_call(
        kernel,
        out_shape=jax.ShapeDtypeStruct((2, 2, SIDE, 1024), jnp.float32),
        in_specs=[pl.BlockSpec(memory_space=pl.ANY), vmem],
        out_specs=vmem,
        scratch_shapes=[
            pltpu.VMEM((STA, WIN, LEN), jnp.bfloat16),
            pltpu.VMEM((2 * SLOTS, LEN), jnp.bfloat16),
            pltpu.VMEM((8, WIN), jnp.int32),
            pltpu.VMEM((WIN, WIN), jnp.int32),
            pltpu.VMEM((2, WIN), jnp.int32),
            pltpu.VMEM((STA, WIN), jnp.float32),
            pltpu.VMEM((PART * SLOTS, WIN), jnp.float32),
            pltpu.VMEM((PART * SLOTS, WIN), jnp.float32),
            pltpu.VMEM((PLANE, STA, 2 * WIN), jnp.bfloat16),
            pltpu.VMEM((Y, 2, 16, STA, 2 * WIN), jnp.bfloat16),
            pltpu.VMEM((2 * ROWS, 2048), jnp.bfloat16),
            pltpu.VMEM((3, 2, ROWS, ROWS), jnp.float32),
            pltpu.VMEM((Y, 2, WIN), jnp.int32),
            pltpu.VMEM((PLANE, Y, 2, WIN), jnp.int32),
            pltpu.VMEM((PLANE, 1024), jnp.int32),
            pltpu.VMEM((1024, 1024), jnp.bfloat16),
            pltpu.VMEM((ROWS, 1024), jnp.float32),
            pltpu.VMEM((3, 2, SIDE, ROWS), jnp.int16),
            pltpu.VMEM((3, 2, SIDE, ROWS), jnp.int16),
            pltpu.VMEM((2, 2, SIDE, ROWS), jnp.int16),
            pltpu.VMEM((2, 2, SIDE, ROWS), jnp.int16),
            pltpu.VMEM((4, 2, ROWS), jnp.float32),
            pltpu.VMEM((4, 2, ROWS), jnp.float32),
            pltpu.VMEM((2, 2, ROWS), jnp.float32),
            pltpu.VMEM((2, 2, ROWS), jnp.float32),
            dma((CHUNKS,)), dma((CHUNKS, PLANE)), dma((CHUNKS, PLANE)),
            dma((Y,)), dma((Y,)), dma((PLANE,)), dma((PLANE,)),
            dma((len(UP),)), dma((len(UP),)), dma((len(DOWN),)), dma((len(DOWN),)),
            dma((3, 4)), dma((3, 4)), dma((2, 2)), dma((2, 2)),
        ],
        compiler_params=pltpu.CompilerParams(
            collective_id=0, has_side_effects=True, vmem_limit_bytes=48 << 20),
    )(records, flags)


def local(records, gap_flags, station_mask):
    return stack_up(records, gap_flags.T * station_mask[None])


def solution(mesh):
    placed = (P("freq", "tm", None), P("freq", "tm"), P("freq"))
    return jax.shard_map(
        local, mesh=mesh, in_specs=placed, out_specs=P("freq", None, "tm", None), check_vma=False
    )
```
